8 devices in a mesh: dz: 2 (over z, y), dy: 2 (over x), dx: 2 (over core).
Axes of the slice: x: 2, y: 2, z: 1, core: 2. Of those that a mesh axis runs over, the one named last changes fastest.
Arguments:
- g_emb: float32 [8, 2048, 768], P(('dz', 'dy', 'dx'))
- g_attn: float32 [8, 1, 4, 768, 768], P(('dz', 'dy', 'dx'))
- g_in: float32 [8, 1, 768, 3072], P(('dz', 'dy', 'dx'))
- g_out: float32 [8, 1, 3072, 768], P(('dz', 'dy', 'dx'))
- g_vecd: float32 [8, 1, 9, 768], P(('dz', 'dy', 'dx'))
- g_vecf: float32 [8, 1, 3072], P(('dz', 'dy', 'dx'))
- opt_m: float32 [8660992], P(('dz', 'dy', 'dx'))
- opt_v: float32 [8660992], P(('dz', 'dy', 'dx'))
- master: float32 [8660992], P(('dz', 'dy', 'dx'))
- tok_ids: int32 [131072], P(('dz', 'dy', 'dx'))
- act_in: bfloat16 [131072, 768], P(('dz', 'dy', 'dx'))
Outputs:
- output 1: float32 [8660992], P(('dz', 'dy', 'dx'))
- output 2: float32 [8660992], P(('dz', 'dy', 'dx'))
- output 3: float32 [8660992], P(('dz', 'dy', 'dx'))
- output 4: bfloat16 [2048, 768], replicated
- output 5: bfloat16 [1, 4, 768, 768], replicated
- output 6: bfloat16 [1, 768, 3072], replicated
- output 7: bfloat16 [1, 3072, 768], replicated
- output 8: bfloat16 [1, 9, 768], replicated
- output 9: bfloat16 [1, 3072], replicated
- output 10: bfloat16 [131072, 768], P(('dz', 'dy', 'dx'))
All inputs are finite; a program needn't handle non-finite values.
Results may differ from the reference program's by a relative error of at most 0.001.
Values are sent between devices in bfloat16 or wider.
A program may use at most 1 GiB of HBM per device.

```python
import math
import jax
import jax.numpy as jnp
from jax import lax

D = 768
FF = 3072
LAYERS = 1
VOCAB = 2048
TOKENS_DEV = 16384
DEVICES = 8
ADAM_STEP = 2

LEARN_RATE = 0.002
BETA_ONE = 0.9
BETA_TWO = 0.95
ADAM_EPS = 1e-8
PARAM_COUNT = VOCAB * D + LAYERS * (4 * D * D + 2 * D * FF + 9 * D + FF)
PADDED_COUNT = -(-PARAM_COUNT // (128 * DEVICES)) * (128 * DEVICES)
TENSOR_SHAPES = [(VOCAB, D), (LAYERS, 4, D, D), (LAYERS, D, FF), (LAYERS, FF, D), (LAYERS, 9, D), (LAYERS, FF)]
ARG_NAMES = ["g_emb", "g_attn", "g_in", "g_out", "g_vecd", "g_vecf"]


def setup_inputs(seed: int = 0) -> dict:
    rand_keys = jax.random.split(jax.random.key(seed), 12)
    dev_scale = jax.random.uniform(rand_keys[0], (DEVICES,), jnp.float32, 0.5, 1.5) * math.sqrt(DEVICES)
    inputs = {}
    for tensor_index, tensor_shape in enumerate(TENSOR_SHAPES):
        grad_noise = jax.random.normal(rand_keys[1 + tensor_index], (DEVICES,) + tensor_shape, jnp.float32)
        inputs[ARG_NAMES[tensor_index]] = grad_noise * dev_scale.reshape((DEVICES,) + (1,) * len(tensor_shape))
    weight_scales = [D ** -0.5, D ** -0.5, D ** -0.5, FF ** -0.5, 0.2, 0.3]
    scale_parts = [jnp.full((math.prod(tensor_shape),), weight_scale, jnp.float32) for tensor_shape, weight_scale in zip(TENSOR_SHAPES, weight_scales)]
    scale_parts.append(jnp.full((PADDED_COUNT - PARAM_COUNT,), 0.1, jnp.float32))
    m_noise = jax.random.normal(rand_keys[7], (PADDED_COUNT,), jnp.float32)
    v_noise = jax.random.normal(rand_keys[8], (PADDED_COUNT,), jnp.float32)
    w_noise = jax.random.normal(rand_keys[9], (PADDED_COUNT,), jnp.float32)
    inputs["opt_m"] = 0.1 * m_noise
    inputs["opt_v"] = 0.05 * (v_noise * v_noise + 0.25)
    inputs["master"] = w_noise * jnp.concatenate(scale_parts)
    tok_ids = jax.random.randint(rand_keys[10], (DEVICES * TOKENS_DEV,), 0, VOCAB, jnp.int32)
    inputs["tok_ids"] = tok_ids.at[0].set(0).at[1].set(VOCAB - 1)
    inputs["act_in"] = jax.random.normal(rand_keys[11], (DEVICES * TOKENS_DEV, D), jnp.float32).astype(jnp.bfloat16)
    return inputs


def ffn_block(wb_emb, w_in, b_in, w_out, b_out, tok_ids, act_in):
    emb_rows = jnp.take(wb_emb, tok_ids, axis=0).astype(jnp.float32)
    hidden = (emb_rows * math.sqrt(D) + act_in.astype(jnp.float32)).astype(jnp.bfloat16)
    pre_act = jnp.dot(hidden, w_in, preferred_element_type=jnp.float32) + b_in.astype(jnp.float32)
    inner_act = jax.nn.gelu(pre_act, approximate=True).astype(jnp.bfloat16)
    return (jnp.dot(inner_act, w_out, preferred_element_type=jnp.float32) + b_out.astype(jnp.float32)).astype(jnp.bfloat16)


def reference(g_emb, g_attn, g_in, g_out, g_vecd, g_vecf, opt_m, opt_v, master, tok_ids, act_in):
    grad_list = [g_emb, g_attn, g_in, g_out, g_vecd, g_vecf]
    flat_grad = jnp.concatenate([jnp.sum(grad_arr, axis=0).reshape(-1) for grad_arr in grad_list]) / DEVICES
    flat_grad = jnp.pad(flat_grad, (0, PADDED_COUNT - PARAM_COUNT))
    m_new = BETA_ONE * opt_m + (1.0 - BETA_ONE) * flat_grad
    v_new = BETA_TWO * opt_v + (1.0 - BETA_TWO) * flat_grad * flat_grad
    m_hat = m_new / (1.0 - BETA_ONE ** ADAM_STEP)
    v_hat = v_new / (1.0 - BETA_TWO ** ADAM_STEP)
    w_new = master - LEARN_RATE * m_hat / (jnp.sqrt(v_hat) + ADAM_EPS)
    w_half = w_new.astype(jnp.bfloat16)
    pieces = []
    offset = 0
    for tensor_shape in TENSOR_SHAPES:
        elem_count = math.prod(tensor_shape)
        pieces.append(w_half[offset:offset + elem_count].reshape(tensor_shape))
        offset = offset + elem_count
    wb_emb, wb_attn, wb_in, wb_out, wb_vecd, wb_vecf = pieces
    tok_blocks = tok_ids.reshape(DEVICES, TOKENS_DEV)
    act_blocks = act_in.reshape(DEVICES, TOKENS_DEV, D)

    def token_block(tok_pair):
        return ffn_block(wb_emb, wb_in[0], wb_vecf[0], wb_out[0], wb_vecd[0, 8], tok_pair[0], tok_pair[1])

    y_blocks = lax.map(token_block, (tok_blocks, act_blocks))
    y_out = y_blocks.reshape(DEVICES * TOKENS_DEV, D)
    return (m_new, v_new, w_new, wb_emb, wb_attn, wb_in, wb_out, wb_vecd, wb_vecf, y_out)
```

```python
import functools
import math
import jax
import jax.numpy as jnp
from jax import lax
from jax.experimental import pallas as pl
from jax.experimental.pallas import tpu as pltpu
from jax.sharding import PartitionSpec as P

LEARN_RATE = 0.002
BETA_ONE = 0.9
BETA_TWO = 0.95
ADAM_EPS = 1e-8
ADAM_STEP = 2
AXES = ("dz", "dy", "dx")
GRAD_RANKS = (3, 5, 4, 4, 4, 3)
MESH = pl.DeviceIdType.MESH

D = 768
FF = 3072
VOCAB = 2048
NCH = 11
TPC = 96
CROWS = 768
PART = NCH * CROWS
OWN = 8458
HEAD = 80
BOUNDS = (0, 16, 40, 64, 88)


def adam_math(grad, m_old, v_old, w_old):
    m_new = BETA_ONE * m_old + (1.0 - BETA_ONE) * grad
    v_new = BETA_TWO * v_old + (1.0 - BETA_TWO) * grad * grad
    m_hat = m_new / (1.0 - BETA_ONE ** ADAM_STEP)
    v_hat = v_new / (1.0 - BETA_TWO ** ADAM_STEP)
    w_new = w_old - LEARN_RATE * m_hat / (jnp.sqrt(v_hat) + ADAM_EPS)
    return m_new, v_new, w_new


def comm_kernel(g_emb, g_attn, g_in, g_out, m_in, v_in, w_in, frag, vec,
                m_out, v_out, w_out, wb_all, wvec_out,
                rc, own, r1, r2, g_flat, w_flat, m_vm, v_vm, w_vm, wbuf, vecs, wvec,
                d2d_s, d2d_r, own_sem, s1_s, s1_r, s2_s, s2_r,
                as_s, as_r, af_s, af_r, ac_s, ac_r, wloc, ld_sem, st_sem,
                fr_s, fr_r, gt_s, gt_r, vc_s, vc_r, wv_s, wv_r, wv_loc):
    dz, dy, dx = lax.axis_index("dz"), lax.axis_index("dy"), lax.axis_index("dx")
    me = dz * 4 + dy * 2 + dx
    first = jnp.where(dx == 0, dz, dy)
    second = jnp.where(dx == 0, dy, dz)
    p_first = (jnp.where(dx == 0, 1 - dz, dz), jnp.where(dx == 0, dy, 1 - dy), dx)
    p_second = (jnp.where(dx == 0, dz, 1 - dz), jnp.where(dx == 0, 1 - dy, dy), dx)
    p_core = (dz, dy, 1 - dx)

    def coords(index):
        return (index // 4, lax.rem(index // 2, 2), lax.rem(index, 2))

    def part_of(core, a, b):
        f = jnp.where(core == 0, dz, dy)
        s = jnp.where(core == 0, dy, dz)
        f = f if a == 0 else 1 - f
        s = s if b == 0 else 1 - s
        return jnp.where(core == 0, f * 4 + s * 2, s * 4 + f * 2 + 1)

    mine = [part_of(dx, a, b) for a in (0, 1) for b in (0, 1)]
    theirs = [part_of(1 - dx, a, b) for a in (0, 1) for b in (0, 1)]
    shift = me * 10

    barrier = pltpu.get_barrier_semaphore()
    for other in range(1, 8):
        pl.semaphore_signal(barrier, inc=1, device_id=coords(lax.rem(me + other, 8)), device_id_type=MESH)

    loads = []
    for n, (src, dst) in enumerate(((m_in, m_vm), (v_in, v_vm), (w_in, w_vm))):
        loads.append(pltpu.make_async_copy(src, dst.at[pl.ds(HEAD, OWN)], ld_sem.at[n]))
        loads[-1].start()

    def from_grad(part, j, go):
        gchunk = part * NCH + j
        for n, ref in enumerate((g_emb, g_attn, g_in, g_out)):
            @pl.when((gchunk >= BOUNDS[n]) & (gchunk < BOUNDS[n + 1]))
            def _():
                go(ref.at[pl.ds((gchunk - BOUNDS[n]) * TPC, TPC)])

    def own_load(j):
        slot = lax.rem(j, 2)
        for q in range(4):
            from_grad(mine[q], j, lambda src: pltpu.make_async_copy(src, own.at[slot, q], own_sem.at[slot, q]).start())

    def d2d(j, q, src):
        return pltpu.make_async_remote_copy(
            src_ref=src, dst_ref=rc.at[j, q], send_sem=d2d_s.at[j, q], recv_sem=d2d_r.at[j, q],
            device_id=p_core, device_id_type=MESH)

    def d2d_send(j):
        for q in range(4):
            from_grad(theirs[q], j, lambda src: d2d(j, q, src).start())

    def step_one(j):
        return pltpu.make_async_remote_copy(
            src_ref=rc.at[j, pl.ds(2, 2)], dst_ref=r1.at[j], send_sem=s1_s.at[j], recv_sem=s1_r.at[j],
            device_id=p_first, device_id_type=MESH)

    def step_two(j):
        return pltpu.make_async_remote_copy(
            src_ref=r1.at[j, 1], dst_ref=r2.at[j], send_sem=s2_s.at[j], recv_sem=s2_r.at[j],
            device_id=p_second, device_id_type=MESH)

    def gather(j, part, src, target, sends, recvs):
        return pltpu.make_async_remote_copy(
            src_ref=src, dst_ref=wb_all.at[part * NCH + j], send_sem=sends, recv_sem=recvs,
            device_id=target, device_id_type=MESH)

    def frag_copy(n, dst):
        return pltpu.make_async_remote_copy(
            src_ref=frag.at[pl.ds(HEAD * n, HEAD)], dst_ref=dst.at[pl.ds(0, HEAD)],
            send_sem=fr_s.at[n], recv_sem=fr_r.at[n],
            device_id=coords(jnp.minimum(me + 1, 7)), device_id_type=MESH)

    def tail_copy():
        return pltpu.make_async_remote_copy(
            src_ref=g_flat.at[pl.ds(HEAD, 80)], dst_ref=g_flat.at[pl.ds(HEAD + PART, 80)],
            send_sem=gt_s, recv_sem=gt_r,
            device_id=coords(jnp.maximum(me - 1, 0)), device_id_type=MESH)

    def vec_copy(index):
        return pltpu.make_async_remote_copy(
            src_ref=vec, dst_ref=vecs.at[index], send_sem=vc_s, recv_sem=vc_r.at[index],
            device_id=coords(jnp.int32(7)), device_id_type=MESH)

    def wvec_copy(n):
        return pltpu.make_async_remote_copy(
            src_ref=wvec, dst_ref=wvec, send_sem=wv_s.at[n], recv_sem=wv_r,
            device_id=coords(jnp.int32(n)), device_id_type=MESH)

    def out_copies(row, rows, n0):
        return [pltpu.make_async_copy(src.at[pl.ds(HEAD + row, rows)], dst.at[pl.ds(row, rows)], st_sem.at[n0, n])
                for n, (src, dst) in enumerate(((m_vm, m_out), (v_vm, v_out), (w_vm, w_out)))]

    own_load(0)
    own_load(1)
    pl.semaphore_wait(barrier, 7)
    for j in range(3):
        d2d_send(jnp.int32(j))

    @pl.when(me < 7)
    def _():
        for n, dst in enumerate((m_vm, v_vm, w_vm)):
            frag_copy(n, dst).start()
        vec_copy(me).start()

    def add_tiles(dst, src, tiles, per):
        def body(i, _):
            at = pl.ds(i * per, per)
            dst[at] = dst[at] + src[at]
            return 0
        lax.fori_loop(0, tiles // per, body, 0)

    def stage_a(j):
        slot = lax.rem(j, 2)

        @pl.when(j + 3 < NCH)
        def _():
            d2d_send(j + 3)
        for q in (2, 3, 0, 1):
            pltpu.make_async_copy(own.at[slot, q], own.at[slot, q], own_sem.at[slot, q]).wait()
            d2d(j, q, rc.at[j, q]).wait_recv()
            add_tiles(rc.at[j, q], own.at[slot, q], TPC, 8)
            if q == 3:
                step_one(j).start()

        @pl.when(j + 2 < NCH)
        def _():
            own_load(j + 2)

    def stage_b(j):
        step_one(j).wait_recv()
        add_tiles(r1.at[j, 1], rc.at[j, 1], TPC, 8)
        step_two(j).start()
        add_tiles(r1.at[j, 0], rc.at[j, 0], TPC, 8)

    def adam_rows(t, rows, store):
        at = pl.ds(pl.multiple_of(t, 8), rows)
        moved = pl.ds(t + shift, rows)
        m_new, v_new, w_new = adam_math(g_flat[moved, :], m_vm[at, :], v_vm[at, :], w_vm[at, :])
        if store:
            m_vm[at, :] = m_new
            v_vm[at, :] = v_new
            w_vm[at, :] = w_new
        w_flat[moved, :] = w_new

    def tail_sums():
        @pl.when(me < 7)
        def _():
            tail_copy().wait_recv()

        @pl.when(me == 7)
        def _():
            for n in range(7):
                vec_copy(n).wait_recv()
            pltpu.make_async_copy(vec, vecs.at[7], wv_loc).start()
            pltpu.make_async_copy(vec, vecs.at[7], wv_loc).wait()
            total = vecs[0]
            for n in range(1, 8):
                total = total + vecs[n]
            g_flat[pl.ds(HEAD + PART, 80), :] = total * 0.125

    def stage_c(j):
        step_two(j).wait_recv()
        gchunk = me * NCH + j
        is_in = (gchunk >= BOUNDS[2]) & (gchunk < BOUNDS[3])
        base = HEAD + j * CROWS

        def to_flat(width, bands):
            def body(b, _):
                for c in range(width):
                    i = b * width + c
                    g_flat[pl.ds(base + b * (8 * width) + c, 8, stride=width), :] = (r2[j, i] + r1[j, 0, i]) * 0.125
                return 0
            lax.fori_loop(0, bands, body, 0)

        def to_tiles(width, bands):
            def body(b, _):
                for c in range(width):
                    rows = w_flat[pl.ds(base + b * (8 * width) + c, 8, stride=width), :]
                    wbuf[j, b * width + c] = rows.astype(jnp.bfloat16)
                return 0
            lax.fori_loop(0, bands, body, 0)

        @pl.when(is_in)
        def _():
            to_flat(24, 4)

        @pl.when(jnp.logical_not(is_in))
        def _():
            to_flat(6, 16)

        @pl.when(j == 0)
        def _():
            for load in loads:
                load.wait()

            @pl.when(me > 0)
            def _():
                for n, dst in enumerate((m_vm, v_vm, w_vm)):
                    frag_copy(n, dst).wait_recv()
                tail_copy().start()

        @pl.when(j == NCH - 1)
        def _():
            tail_sums()
        start = (base - shift) // 8 * 8

        def adam_body(i, _):
            adam_rows(start + i * 32, 32, True)
            return 0
        lax.fori_loop(0, CROWS // 32, adam_body, 0)
        adam_rows(start + CROWS, 8, False)

        @pl.when(is_in)
        def _():
            to_tiles(24, 4)

        @pl.when(jnp.logical_not(is_in))
        def _():
            to_tiles(6, 16)

        gather(j, me, wbuf.at[j], p_second, as_s.at[j], as_r.at[j]).start()
        gather(j, me, wbuf.at[j], p_first, af_s.at[j, 0], af_r.at[j, 0]).start()
        gather(j, me, wbuf.at[j], p_core, ac_s.at[j, 0], ac_r.at[j, 0]).start()
        pltpu.make_async_copy(wbuf.at[j], wb_all.at[me * NCH + j], wloc.at[j]).start()

        @pl.when(j >= 1)
        def _():
            for copy in out_copies(pl.multiple_of((j - 1) * CROWS, 8), CROWS, j - 1):
                copy.start()

    def stage_d(j):
        part = mine[1]
        gather(j, part, wbuf.at[j], p_second, as_s.at[j], as_r.at[j]).wait_recv()
        src = wb_all.at[part * NCH + j]
        gather(j, part, src, p_first, af_s.at[j, 1], af_r.at[j, 1]).start()
        gather(j, part, src, p_core, ac_s.at[j, 1], ac_r.at[j, 1]).start()

    def stage_e(j):
        for b in (0, 1):
            part = mine[2 + b]
            src = wb_all.at[part * NCH + j]
            gather(j, part, src, p_first, af_s.at[j, b], af_r.at[j, b]).wait_recv()
            gather(j, part, src, p_core, ac_s.at[j, 2 + b], ac_r.at[j, 2 + b]).start()

    def tail():
        start = (HEAD + PART - shift) // 8 * 8

        def body(i, _):
            adam_rows(start + i * 8, 8, True)
            return 0
        lax.fori_loop(0, (8544 - start) // 8, body, 0)

        @pl.when(me == 7)
        def _():
            wvec[...] = w_flat[pl.ds(HEAD + PART, 80), :].astype(jnp.bfloat16)
            for n in range(7):
                wvec_copy(n).start()
        for copy in out_copies((NCH - 1) * CROWS, OWN - (NCH - 1) * CROWS, NCH - 1):
            copy.start()

    offs = (0, 2, 4, 5, 6)

    def tick(t, _):
        for off, stage in zip(offs, (stage_a, stage_b, stage_c, stage_d, stage_e)):
            j = t - off

            @pl.when((j >= 0) & (j < NCH))
            def _():
                stage(j)
        @pl.when(t - offs[2] == NCH - 1)
        def _():
            tail()
        return 0
    lax.fori_loop(0, NCH + offs[-1], tick, 0)

    @pl.when(me < 7)
    def _():
        wvec_copy(0).wait_recv()
        for n, dst in enumerate((m_vm, v_vm, w_vm)):
            frag_copy(n, dst).wait_send()
        vec_copy(me).wait_send()

    @pl.when(me == 7)
    def _():
        for n in range(7):
            wvec_copy(n).wait_send()

    @pl.when(me > 0)
    def _():
        tail_copy().wait_send()
    wv_copy = pltpu.make_async_copy(wvec, wvec_out, wv_loc)
    wv_copy.start()

    def drain(j, _):
        for q in range(4):
            d2d(j, q, rc.at[j, q]).wait_send()
            gather(j, mine[q], wbuf.at[j], p_core, ac_s.at[j, q], ac_r.at[j, q]).wait()
        step_one(j).wait_send()
        step_two(j).wait_send()
        gather(j, me, wbuf.at[j], p_second, as_s.at[j], as_r.at[j]).wait_send()
        for b in (0, 1):
            gather(j, me, wbuf.at[j], p_first, af_s.at[j, b], af_r.at[j, b]).wait_send()
        pltpu.make_async_copy(wbuf.at[j], wb_all.at[me * NCH + j], wloc.at[j]).wait()
        return 0
    lax.fori_loop(0, NCH, drain, 0)

    def drain_out(j, _):
        for copy in out_copies(0, CROWS, j):
            copy.wait()
        return 0
    lax.fori_loop(0, NCH - 1, drain_out, 0)
    for copy in out_copies((NCH - 1) * CROWS, OWN - (NCH - 1) * CROWS, NCH - 1):
        copy.wait()
    wv_copy.wait()


def comm_call(grads, m_in, v_in, w_in, frag, vec):
    any_spec = pl.BlockSpec(memory_space=pl.ANY)
    f32, dma = jnp.float32, pltpu.SemaphoreType.DMA
    flat = jax.ShapeDtypeStruct((OWN, 128), f32)
    return pl.pallas_call(
        comm_kernel,
        out_shape=(flat, flat, flat,
                   jax.ShapeDtypeStruct((8 * NCH, TPC, 8, 128), jnp.bfloat16),
                   jax.ShapeDtypeStruct((80, 128), jnp.bfloat16)),
        in_specs=[any_spec] * 9,
        out_specs=[any_spec] * 5,
        scratch_shapes=[
            pltpu.VMEM((NCH, 4, TPC, 8, 128), f32),
            pltpu.VMEM((2, 4, TPC, 8, 128), f32),
            pltpu.VMEM((NCH, 2, TPC, 8, 128), f32),
            pltpu.VMEM((NCH, TPC, 8, 128), f32),
            pltpu.VMEM((8704, 128), f32),
            pltpu.VMEM((8704, 128), f32),
            pltpu.VMEM((8544, 128), f32),
            pltpu.VMEM((8544, 128), f32),
            pltpu.VMEM((8544, 128), f32),
            pltpu.VMEM((NCH, TPC, 8, 128), jnp.bfloat16),
            pltpu.VMEM((8, 80, 128), f32),
            pltpu.VMEM((80, 128), jnp.bfloat16),
            dma((NCH, 4)), dma((NCH, 4)), dma((2, 4)),
            dma((NCH,)), dma((NCH,)), dma((NCH,)), dma((NCH,)),
            dma((NCH,)), dma((NCH,)), dma((NCH, 2)), dma((NCH, 2)), dma((NCH, 4)), dma((NCH, 4)),
            dma((NCH,)), dma((3,)), dma((NCH, 3)),
            dma((3,)), dma((3,)), dma(()), dma(()), dma(()), dma((8,)), dma((7,)), dma(()), dma(()),
        ],
        compiler_params=pltpu.CompilerParams(collective_id=0, has_side_effects=True, vmem_limit_bytes=62 << 20),
        name="adam_exchange",
    )(*grads, m_in, v_in, w_in, frag, vec)


TM = 512
FCH = 512


def ffn_kernel(ids, act, emb_t, win, wout, b_in, b_out, y_ref, table, rows):
    @pl.when(pl.program_id(0) == 0)
    def _():
        def fill(b, _):
            for c in range(6):
                tile = emb_t[b * 6 + c].astype(jnp.float32) * math.sqrt(D)
                table[pl.ds(b * 64 + c, 8, stride=8), :] = tile
            return 0
        lax.fori_loop(0, VOCAB // 8, fill, 0)

    def pick(i, _):
        for k in range(16):
            r = i * 16 + k
            tok = ids[0, 0, r]
            rows[pl.ds(pl.multiple_of(r * 8, 8), 8), :] = table[pl.ds(pl.multiple_of(tok * 8, 8), 8), :]
        return 0
    lax.fori_loop(0, TM // 16, pick, 0)
    h = jnp.concatenate(
        [(rows[pl.ds(c, TM, stride=8), :] + act[:, c * 128:(c + 1) * 128].astype(jnp.float32)).astype(jnp.bfloat16)
         for c in range(6)], axis=1)
    inner = []
    for f in range(FF // FCH):
        at = slice(f * FCH, (f + 1) * FCH)
        pre = jnp.dot(h, win[:, at], preferred_element_type=jnp.float32) + b_in[:, at].astype(jnp.float32)
        inner.append(jax.nn.gelu(pre, approximate=True).astype(jnp.bfloat16))
    u = jnp.concatenate(inner, axis=1)
    out = jnp.dot(u, wout[...], preferred_element_type=jnp.float32) + b_out[...].astype(jnp.float32)
    y_ref[...] = out.astype(jnp.bfloat16)


def ffn_call(tok_ids, act_in, emb_t, win, wout, b_in, b_out):
    steps = act_in.shape[0] // TM
    const = lambda shape: pl.BlockSpec(shape, lambda i: (0,) * len(shape), pipeline_mode=pl.Buffered(1))
    return pl.pallas_call(
        ffn_kernel,
        grid=(steps,),
        out_shape=jax.ShapeDtypeStruct(act_in.shape, jnp.bfloat16),
        in_specs=[
            pl.BlockSpec((1, 1, TM), lambda i: (i, 0, 0), memory_space=pltpu.SMEM),
            pl.BlockSpec((TM, D), lambda i: (i, 0)),
            const((VOCAB * D // 1024, 8, 128)), const((D, FF)), const((FF, D)), const((1, FF)), const((1, D)),
        ],
        out_specs=pl.BlockSpec((TM, D), lambda i: (i, 0)),
        scratch_shapes=[pltpu.VMEM((VOCAB * 8, 128), jnp.float32), pltpu.VMEM((TM * 8, 128), jnp.float32)],
        compiler_params=pltpu.CompilerParams(dimension_semantics=("arbitrary",), vmem_limit_bytes=62 << 20),
        name="gather_ffn",
    )(tok_ids.reshape(steps, 1, TM), act_in, emb_t, win, wout, b_in, b_out)


def to_tiles(arr):
    rows, cols = arr.shape
    return arr.reshape(rows // 8, 8, cols // 128, 128).transpose(0, 2, 1, 3).reshape(rows * cols // 1024, 8, 128)


def from_tiles(tiles, rows, cols):
    return tiles.reshape(rows // 8, cols // 128, 8, 128).transpose(0, 2, 1, 3).reshape(rows, cols)


def solution(mesh):
    def device_step(g_emb, g_attn, g_in, g_out, g_vecd, g_vecf, opt_m, opt_v, master, tok_ids, act_in):
        grads = [to_tiles(g_emb[0]), to_tiles(g_attn.reshape(4 * D, D)), to_tiles(g_in[0, 0]), to_tiles(g_out[0, 0])]
        vec = jnp.concatenate([g_vecd.reshape(-1), g_vecf.reshape(-1), jnp.zeros((256,), jnp.float32)]).reshape(80, 128)
        state = [opt_m, opt_v, master]
        frag = jnp.concatenate([arr[-HEAD * 128:] for arr in state]).reshape(3 * HEAD, 128)
        m_new, v_new, w_new, wb_all, wvec = comm_call(grads, *[arr.reshape(OWN, 128) for arr in state], frag, vec)
        tiles = [wb_all[BOUNDS[n]:BOUNDS[n + 1]].reshape(-1, 8, 128) for n in range(4)]
        wb_emb = from_tiles(tiles[0], VOCAB, D)
        wb_attn = from_tiles(tiles[1], 4 * D, D).reshape(1, 4, D, D)
        wb_in = from_tiles(tiles[2], D, FF)
        wb_out = from_tiles(tiles[3], FF, D)
        vec_flat = wvec.reshape(-1)
        wb_vecd = vec_flat[:9 * D].reshape(1, 9, D)
        wb_vecf = vec_flat[9 * D:9 * D + FF].reshape(1, FF)
        y_out = ffn_call(tok_ids, act_in, tiles[0], wb_in, wb_out, wb_vecf, wb_vecd[0, 8:9])
        return (m_new.reshape(-1), v_new.reshape(-1), w_new.reshape(-1), wb_emb, wb_attn, wb_in[None], wb_out[None],
                wb_vecd, wb_vecf, y_out)

    grad_specs = tuple(P(AXES, *([None] * (grad_rank - 1))) for grad_rank in GRAD_RANKS)
    in_specs = grad_specs + (P(AXES), P(AXES), P(AXES), P(AXES), P(AXES, None))
    out_specs = (P(AXES), P(AXES), P(AXES), P(), P(), P(), P(), P(), P(), P(AXES, None))
    return jax.shard_map(device_step, mesh=mesh, in_specs=in_specs, out_specs=out_specs, check_vma=False)
```

```python
import functools
import math
import jax
import jax.numpy as jnp
from jax import lax
from jax.experimental import pallas as pl
from jax.experimental.pallas import tpu as pltpu
from jax.sharding import PartitionSpec as P

LEARN_RATE = 0.002
BETA_ONE = 0.9
BETA_TWO = 0.95
ADAM_EPS = 1e-8
ADAM_STEP = 2
AXES = ("dz", "dy", "dx")
GRAD_RANKS = (3, 5, 4, 4, 4, 3)
MESH = pl.DeviceIdType.MESH

D = 768
FF = 3072
VOCAB = 2048
NCH = 22
TPC = 48
CROWS = 384
PART = NCH * CROWS
OWN = 8458
HEAD = 80
BOUNDS = (0, 32, 80, 128, 176)
OFFS = (0, 2, 4, 5, 6)
GROWS = 8784
SLOTS = 4 * NCH


def adam_math(grad, m_old, v_old, w_old):
    m_new = BETA_ONE * m_old + (1.0 - BETA_ONE) * grad
    v_new = BETA_TWO * v_old + (1.0 - BETA_TWO) * grad * grad
    m_hat = m_new / (1.0 - BETA_ONE ** ADAM_STEP)
    v_hat = v_new / (1.0 - BETA_TWO ** ADAM_STEP)
    w_new = w_old - LEARN_RATE * m_hat / (jnp.sqrt(v_hat) + ADAM_EPS)
    return m_new, v_new, w_new


def coords(index):
    return (index // 4, lax.rem(index // 2, 2), lax.rem(index, 2))


def engine_scratch(slots):
    f32, dma = jnp.float32, pltpu.SemaphoreType.DMA
    return [
        pltpu.VMEM((slots, TPC, 8, 128), f32),
        pltpu.VMEM((2, 4, TPC, 8, 128), f32),
        pltpu.VMEM((2 * NCH, TPC, 8, 128), f32),
        pltpu.VMEM((NCH, TPC, 8, 128), f32),
        pltpu.VMEM((2, CROWS, 128), f32),
        pltpu.VMEM((CROWS, 128), f32),
        pltpu.VMEM((2, 3, HEAD + CROWS, 128), f32),
        pltpu.VMEM((NCH, TPC, 8, 128), jnp.bfloat16),
        dma((slots,)), dma((slots,)), dma((2, 4)),
        dma((2 * NCH,)), dma((2 * NCH,)), dma((NCH,)), dma((NCH,)),
        dma((NCH,)), dma((slots,)), dma((slots,)), dma((slots,)), dma((slots,)),
        dma((NCH,)), dma((2, 3, 2)), dma((2,)), dma(()), dma(()),
    ]


class Engine:
    def __init__(self, grads, state, frag, g_nat, wbs, scratch):
        self.grads, self.state = grads, state
        self.frag, self.g_nat, self.wbs = frag, g_nat, wbs
        (self.rc, self.own, self.r1, self.r2, self.g_ch, self.w_ch, self.win, self.wbuf,
         self.d2d_s, self.d2d_r, self.own_sem, self.s1_s, self.s1_r, self.s2_s, self.s2_r,
         self.ay_s, self.ax_s, self.ac_s, self.ag_r, self.ac_r,
         self.wloc, self.win_sem, self.g_sem, self.tail_s, self.tail_r) = scratch
        dz, dy, dx = lax.axis_index("dz"), lax.axis_index("dy"), lax.axis_index("dx")
        self.me = dz * 4 + dy * 2 + dx
        self.p_core = (dz, dy, 1 - dx)
        core0 = dx == 0
        self.p_first = (jnp.where(core0, 1 - dz, dz), jnp.where(core0, dy, 1 - dy), dx)
        self.p_second = (jnp.where(core0, dz, 1 - dz), jnp.where(core0, 1 - dy, dy), dx)

        def part_of(is0, a, b):
            f, s = jnp.where(is0, dz, dy), jnp.where(is0, dy, dz)
            f = f if a == 0 else 1 - f
            s = s if b == 0 else 1 - s
            return jnp.where(is0, f * 4 + s * 2, s * 4 + f * 2) + jnp.where(is0 == core0, dx, 1 - dx)

        other0 = dx == 1
        self.mine = [part_of(core0, a, b) for a in (0, 1) for b in (0, 1)]
        self.theirs = [part_of(other0, a, b) for a in (0, 1) for b in (0, 1)]
        self.shift = self.me * 10

    def valid(self, j):
        return (j >= 0) & (j < NCH)

    def slot(self, part, j):
        return part // 2 * NCH + j

    def remote(self, src, dst, send, recv, to):
        return pltpu.make_async_remote_copy(src_ref=src, dst_ref=dst, send_sem=send, recv_sem=recv,
                                            device_id=to, device_id_type=MESH)

    def from_grad(self, part, j, go):
        at = part * NCH + j
        for lo, hi, ref in self.grads:
            @pl.when((at >= lo) & (at < hi))
            def _():
                go(ref.at[pl.ds((at - lo) * TPC, TPC)])

    def to_wb(self, part, j, go):
        at = part * NCH + j
        for lo, hi, ref in self.wbs:
            @pl.when((at >= lo) & (at < hi))
            def _():
                go(ref.at[at - lo])

    def own_load(self, j):
        buf = lax.rem(j, 2)
        for q in range(4):
            self.from_grad(self.mine[q], j, lambda src: pltpu.make_async_copy(
                src, self.own.at[buf, q], self.own_sem.at[buf, q]).start())

    def d2d_send(self, j):
        for part in self.theirs:
            s = self.slot(part, j)
            self.from_grad(part, j, lambda src: self.remote(
                src, self.rc.at[s], self.d2d_s.at[s], self.d2d_r.at[s], self.p_core).start())

    def landing(self, sem, ref):
        return self.remote(ref, ref, sem, sem, self.p_core)

    def step_one(self, s, b, j):
        n = b * NCH + j
        return self.remote(self.rc.at[s], self.r1.at[n], self.s1_s.at[n], self.s1_r.at[n], self.p_first)

    def step_two(self, j):
        return self.remote(self.r1.at[NCH + j], self.r2.at[j], self.s2_s.at[j], self.s2_r.at[j], self.p_second)

    def tail_copy(self):
        return self.remote(self.g_ch.at[0, pl.ds(0, HEAD)], self.g_nat.at[pl.ds(PART, HEAD)],
                           self.tail_s, self.tail_r, coords(jnp.maximum(self.me - 1, 0)))

    def window(self, j):
        c, buf = j, lax.rem(j, 2)
        rest = [pltpu.make_async_copy(
            src.at[pl.ds(pl.multiple_of(jnp.maximum(c * CROWS - HEAD, 0), 8), HEAD + CROWS)],
            self.win.at[buf, n], self.win_sem.at[buf, n, 0]) for n, src in enumerate(self.state)]
        zero = []
        for n, src in enumerate(self.state):
            zero.append(pltpu.make_async_copy(self.frag.at[pl.ds(HEAD * n, HEAD)], self.win.at[buf, n, pl.ds(0, HEAD)],
                                              self.win_sem.at[buf, n, 0]))
            zero.append(pltpu.make_async_copy(src.at[pl.ds(0, CROWS)], self.win.at[buf, n, pl.ds(HEAD, CROWS)],
                                              self.win_sem.at[buf, n, 1]))
        return c, rest, zero

    def window_do(self, j, what):
        c, rest, zero = self.window(j)

        @pl.when(c > 0)
        def _():
            for copy in rest:
                what(copy)

        @pl.when(c == 0)
        def _():
            for copy in zero:
                what(copy)

    def begin(self):
        self.own_load(jnp.int32(0))
        self.own_load(jnp.int32(1))

    def greet(self):
        barrier = pltpu.get_barrier_semaphore()
        for other in range(1, 8):
            pl.semaphore_signal(barrier, inc=1, device_id=coords(lax.rem(self.me + other, 8)), device_id_type=MESH)
        self.begin()
        pl.semaphore_wait(barrier, 7)
        for j in range(3):
            self.d2d_send(jnp.int32(j))

    def add_tiles(self, dst, src):
        def body(i, _):
            at = pl.ds(i * 8, 8)
            dst[at] = dst[at] + src[at]
            return 0
        lax.fori_loop(0, TPC // 8, body, 0)

    def stage_a(self, j):
        buf = lax.rem(j, 2)

        @pl.when(j + 3 < NCH)
        def _():
            self.d2d_send(j + 3)
        for q in (2, 3, 0, 1):
            s = self.slot(self.mine[q], j)
            pltpu.make_async_copy(self.own.at[buf, q], self.own.at[buf, q], self.own_sem.at[buf, q]).wait()
            self.landing(self.d2d_r.at[s], self.rc.at[s]).wait_recv()
            self.add_tiles(self.rc.at[s], self.own.at[buf, q])
            if q >= 2:
                self.step_one(s, q - 2, j).start()

        @pl.when(j + 2 < NCH)
        def _():
            self.own_load(j + 2)

    def stage_b(self, j):
        for b in (1, 0):
            s = self.slot(self.mine[b], j)
            self.step_one(s, b, j).wait_recv()
            self.add_tiles(self.r1.at[b * NCH + j], self.rc.at[s])
            if b == 1:
                self.step_two(j).start()

    def stage_c(self, j):
        me, s, i, c = self.me, self.slot(self.me, j), j, j
        buf = lax.rem(i, 2)
        at = me * NCH + c
        is_in = (at >= BOUNDS[2]) & (at < BOUNDS[3])
        g_store = pltpu.make_async_copy(self.g_ch.at[buf], self.g_nat.at[pl.ds(pl.multiple_of(c * CROWS, 8), CROWS)],
                                        self.g_sem.at[buf])
        self.step_two(j).wait_recv()

        @pl.when(i >= 2)
        def _():
            g_store.wait()

        @pl.when((i == 2) & (me > 0))
        def _():
            self.tail_copy().wait_send()

        def to_flat(width):
            def body(b, _):
                for n in range(width):
                    t = b * width + n
                    self.g_ch[buf, pl.ds(b * (8 * width) + n, 8, stride=width), :] = (
                        self.r2[i, t] + self.r1[i, t]) * 0.125
                return 0
            lax.fori_loop(0, TPC // width, body, 0)

        def to_tiles(width):
            def body(b, _):
                for n in range(width):
                    rows = self.w_ch[pl.ds(b * (8 * width) + n, 8, stride=width), :]
                    self.wbuf[i, b * width + n] = rows.astype(jnp.bfloat16)
                return 0
            lax.fori_loop(0, TPC // width, body, 0)

        @pl.when(is_in)
        def _():
            to_flat(24)

        @pl.when(jnp.logical_not(is_in))
        def _():
            to_flat(6)
        g_store.start()

        @pl.when((c == 0) & (me > 0))
        def _():
            self.tail_copy().start()
        self.window_do(j, lambda copy: copy.wait())

        def body(n, _):
            at = pl.ds(pl.multiple_of(n * 32, 8), 32)
            old = pl.ds(HEAD - self.shift + n * 32, 32)
            self.w_ch[at, :] = adam_math(self.g_ch[buf, at, :], self.win[buf, 0, old, :], self.win[buf, 1, old, :],
                                         self.win[buf, 2, old, :])[2]
            return 0
        lax.fori_loop(0, CROWS // 32, body, 0)

        @pl.when(is_in)
        def _():
            to_tiles(24)

        @pl.when(jnp.logical_not(is_in))
        def _():
            to_tiles(6)

        def send(dst):
            src = self.wbuf.at[i]
            self.remote(src, dst, self.ay_s.at[i], self.ag_r.at[s], self.p_second).start()
            self.remote(src, dst, self.ax_s.at[s], self.ag_r.at[s], self.p_first).start()
            self.remote(src, dst, self.ac_s.at[s], self.ac_r.at[s], self.p_core).start()
            pltpu.make_async_copy(src, dst, self.wloc.at[i]).start()
        self.to_wb(me, j, send)

    def stage_d(self, j):
        part = self.mine[1]
        s = self.slot(part, j)
        self.landing(self.ag_r.at[s], self.wbs[0][2].at[0]).wait_recv()

        def send(ref):
            self.remote(ref, ref, self.ax_s.at[s], self.ag_r.at[s], self.p_first).start()
            self.remote(ref, ref, self.ac_s.at[s], self.ac_r.at[s], self.p_core).start()
        self.to_wb(part, j, send)

    def stage_e(self, j):
        for part in (self.mine[2], self.mine[3]):
            s = self.slot(part, j)
            self.landing(self.ag_r.at[s], self.wbs[0][2].at[0]).wait_recv()
            self.to_wb(part, j, lambda ref: self.remote(
                ref, ref, self.ac_s.at[s], self.ac_r.at[s], self.p_core).start())

    def tick(self, t):
        for off, stage in zip(OFFS, (self.stage_a, self.stage_b, self.stage_c, self.stage_d, self.stage_e)):
            @pl.when(self.valid(t - off))
            def _():
                stage(t - off)
            if off == OFFS[2]:
                @pl.when(self.valid(t + 1 - off))
                def _():
                    self.window_do(t + 1 - off, lambda copy: copy.start())

    def drain(self):
        tile = self.wbs[0][2].at[0]

        def body(j, _):
            for part in self.theirs:
                s = self.slot(part, j)
                self.landing(self.d2d_s.at[s], self.rc.at[s]).wait_send()
                self.landing(self.ac_r.at[s], tile).wait_recv()
            for q, part in enumerate(self.mine):
                s = self.slot(part, j)
                self.landing(self.ac_s.at[s], tile).wait_send()
                if q >= 2:
                    self.step_one(s, q - 2, j).wait_send()
                else:
                    self.landing(self.ax_s.at[s], tile).wait_send()
            self.step_two(j).wait_send()
            self.landing(self.ay_s.at[j], tile).wait_send()
            pltpu.make_async_copy(tile, tile, self.wloc.at[j]).wait()
            return 0
        lax.fori_loop(0, NCH, body, 0)
        for buf in range(2):
            pltpu.make_async_copy(self.g_ch.at[buf], self.g_ch.at[buf], self.g_sem.at[buf]).wait()

        @pl.when(self.me < 7)
        def _():
            self.tail_copy().wait_recv()


def exchange_kernel(g_emb, g_attn, g_in, g_out, m_in, v_in, w_in, frag, vec,
                 g_nat, wb_emb, wb_attn, wb_in, wb_out, wvec_out, frag_got,
                 vecs, wvec, vwin, fr_s, fr_r, vc_s, vc_r, wv_s, wv_r, loc, vw_sem, *scratch):
    state = (m_in, v_in, w_in)
    span = lambda refs: [(BOUNDS[n], BOUNDS[n + 1], ref) for n, ref in enumerate(refs)]
    eng = Engine(span((g_emb, g_attn, g_in, g_out)), state, frag_got, g_nat,
                 span((wb_emb, wb_attn, wb_in, wb_out)), scratch)
    me = eng.me
    frag_copy = eng.remote(frag, frag_got, fr_s, fr_r, coords(jnp.minimum(me + 1, 7)))

    def vec_copy(n):
        return eng.remote(vec, vecs.at[n], vc_s, vc_r.at[n], coords(jnp.int32(7)))

    def wvec_copy(n):
        return eng.remote(wvec, wvec, wv_s.at[n], wv_r, coords(jnp.int32(n)))

    rows = OWN - 8368
    vwins = [pltpu.make_async_copy(src.at[pl.ds(8368, rows)], vwin.at[n, pl.ds(0, rows)], vw_sem.at[n])
             for n, src in enumerate(state)]
    eng.greet()

    @pl.when(me < 7)
    def _():
        frag_copy.start()
        vec_copy(me).start()

    @pl.when(me == 7)
    def _():
        for copy in vwins:
            copy.start()
        own_vec = pltpu.make_async_copy(vec, vecs.at[7], loc)
        own_vec.start()
        own_vec.wait()

    def step(t, _):
        @pl.when((t == OFFS[2] - 1) & (me > 0))
        def _():
            frag_copy.wait_recv()
        eng.tick(t)

        @pl.when((t == 8) & (me == 7))
        def _():
            for n in range(7):
                vec_copy(n).wait_recv()
            for copy in vwins:
                copy.wait()
            total = vecs[0]
            for n in range(1, 8):
                total = total + vecs[n]
            total = total * 0.125
            vecs[0] = total
            g_store = pltpu.make_async_copy(vecs.at[0], g_nat.at[pl.ds(PART, HEAD)], loc)
            g_store.start()
            old = pl.ds(10, HEAD)
            wvec[...] = adam_math(total, vwin[0, old, :], vwin[1, old, :], vwin[2, old, :])[2].astype(jnp.bfloat16)
            for n in range(7):
                wvec_copy(n).start()
            g_store.wait()
        return 0
    lax.fori_loop(0, NCH + OFFS[-1], step, 0)

    @pl.when(me < 7)
    def _():
        wvec_copy(0).wait_recv()
        frag_copy.wait_send()
        vec_copy(me).wait_send()

    @pl.when(me == 7)
    def _():
        for n in range(7):
            wvec_copy(n).wait_send()
    wv_store = pltpu.make_async_copy(wvec, wvec_out, loc)
    wv_store.start()
    eng.drain()
    wv_store.wait()


ANY = pl.BlockSpec(memory_space=pl.ANY)


def exchange_call(grads, state, frag, vec):
    f32, dma = jnp.float32, pltpu.SemaphoreType.DMA
    wb = lambda n: jax.ShapeDtypeStruct((BOUNDS[n + 1] - BOUNDS[n], TPC, 8, 128), jnp.bfloat16)
    return pl.pallas_call(
        exchange_kernel,
        out_shape=(jax.ShapeDtypeStruct((GROWS, 128), f32), wb(0), wb(1), wb(2), wb(3),
                   jax.ShapeDtypeStruct((HEAD, 128), jnp.bfloat16), jax.ShapeDtypeStruct((3 * HEAD, 128), f32)),
        in_specs=[ANY] * 9,
        out_specs=[ANY] * 7,
        scratch_shapes=[
            pltpu.VMEM((8, HEAD, 128), f32), pltpu.VMEM((HEAD, 128), jnp.bfloat16), pltpu.VMEM((3, 96, 128), f32),
            dma(()), dma(()), dma(()), dma((8,)), dma((7,)), dma(()), dma(()), dma((3,)),
        ] + engine_scratch(SLOTS),
        compiler_params=pltpu.CompilerParams(collective_id=0, has_side_effects=True, vmem_limit_bytes=62 << 20),
        name="adam_exchange",
    )(*grads, *state, frag, vec)


TM = 512
FCH = 512
STATE_ROWS = 272
GELU_C = math.sqrt(2.0 / math.pi)


def gelu(x):
    half = 0.5 * x
    return half * jnp.tanh(x * (x * x * (GELU_C * 0.044715) + GELU_C)) + half


def ffn_kernel(ids, act, emb_t, win, wout, b_in, b_out, g_ref, m_ref, v_ref, w_ref, *refs):
    copies, (y_ref, m_out, v_out, w_out), dests, (table, rows, h_ref, u_ref) = refs[:4], refs[4:8], refs[8:12], refs[12:]
    step = pl.program_id(0)
    shift = (lax.axis_index("dz") * 4 + lax.axis_index("dy") * 2 + lax.axis_index("dx")) * 10

    def pick_row(r, at):
        tok = ids[0, 0, r]
        rows[at, :] = table[pl.ds(pl.multiple_of(tok * 8, 8), 8), :]

    def build():
        for c in range(6):
            lanes = slice(c * 128, (c + 1) * 128)
            h_ref[:, lanes] = (rows[pl.ds(c, TM, stride=8), :] + act[:, lanes].astype(jnp.float32)).astype(jnp.bfloat16)

    @pl.when(step == 0)
    def _():
        def fill(b, _):
            for c in range(6):
                tile = emb_t[b * 6 + c].astype(jnp.float32) * math.sqrt(D)
                table[pl.ds(b * 64 + c, 8, stride=8), :] = tile
            return 0
        lax.fori_loop(0, VOCAB // 8, fill, 0)

        def pick(i, _):
            for k in range(16):
                r = i * 16 + k
                pick_row(r, pl.ds(pl.multiple_of(r * 8, 8), 8))
            return 0
        lax.fori_loop(0, TM // 16, pick, 0)
        build()

    @pl.when(step > 0)
    def _():
        h = h_ref[...]
        count = FF // FCH
        for f in range(count):
            at = slice(f * FCH, (f + 1) * FCH)
            pre = jnp.dot(h, win[:, at], preferred_element_type=jnp.float32) + b_in[:, at].astype(jnp.float32)
            for r in range(f * TM // count, (f + 1) * TM // count):
                pick_row(r, slice(r * 8, r * 8 + 8))
            u_ref[:, at] = gelu(pre).astype(jnp.bfloat16)
        out = jnp.dot(u_ref[...], wout[...], preferred_element_type=jnp.float32)
        y_ref[...] = (out + b_out[...].astype(jnp.float32)).astype(jnp.bfloat16)
        build()
        for src, dst in zip(copies, dests):
            dst[...] = src[...]
        grad = g_ref[pl.ds((step - 1) * STATE_ROWS + shift, STATE_ROWS), :]
        m_out[...], v_out[...], w_out[...] = adam_math(grad, m_ref[...], v_ref[...], w_ref[...])


def const(shape):
    return pl.BlockSpec(shape, lambda i: (0,) * len(shape), pipeline_mode=pl.Buffered(1))


def ffn_call(tok_ids, act_in, emb_t, win, wout, b_in, b_out, g_nat, state, weights):
    tiles = act_in.shape[0] // TM
    before = lambda rows, cols: pl.BlockSpec((rows, cols), lambda i: (jnp.maximum(i - 1, 0), 0))
    after = lambda i: jnp.minimum(i, tiles - 1)
    passed = [before(arr.shape[0] // tiles, arr.shape[1]) for arr in weights]
    kept = [before(STATE_ROWS, 128)] * 3
    return pl.pallas_call(
        ffn_kernel,
        grid=(tiles + 1,),
        out_shape=[jax.ShapeDtypeStruct(act_in.shape, jnp.bfloat16)]
        + [jax.ShapeDtypeStruct(arr.shape, arr.dtype) for arr in list(state) + list(weights)],
        in_specs=[
            pl.BlockSpec((1, 1, TM), lambda i: (after(i), 0, 0), memory_space=pltpu.SMEM),
            pl.BlockSpec((TM, D), lambda i: (after(i), 0)),
            const((VOCAB * D // 1024, 8, 128)), const((D, FF)), const((FF, D)), const((1, FF)), const((1, D)),
            const((GROWS, 128)),
        ] + kept + passed,
        out_specs=[before(TM, D)] + kept + passed,
        scratch_shapes=[pltpu.VMEM((VOCAB * 8, 128), jnp.float32), pltpu.VMEM((TM * 8, 128), jnp.float32),
                        pltpu.VMEM((TM, D), jnp.bfloat16), pltpu.VMEM((TM, FF), jnp.bfloat16)],
        compiler_params=pltpu.CompilerParams(dimension_semantics=("arbitrary",), vmem_limit_bytes=62 << 20),
        name="ffn_and_state",
    )(tok_ids.reshape(tiles, 1, TM), act_in, emb_t, win, wout, b_in, b_out, g_nat, *state, *weights)


def to_tiles(arr):
    rows, cols = arr.shape
    return arr.reshape(rows // 8, 8, cols // 128, 128).transpose(0, 2, 1, 3).reshape(rows * cols // 1024, 8, 128)


def from_tiles(tiles, rows, cols):
    return tiles.reshape(rows // 8, cols // 128, 8, 128).transpose(0, 2, 1, 3).reshape(rows, cols)


def solution(mesh):
    def device_step(g_emb, g_attn, g_in, g_out, g_vecd, g_vecf, opt_m, opt_v, master, tok_ids, act_in):
        grads = [to_tiles(g_emb[0]), to_tiles(g_attn.reshape(4 * D, D)), to_tiles(g_in[0, 0]), to_tiles(g_out[0, 0])]
        vec = jnp.concatenate([g_vecd.reshape(-1), g_vecf.reshape(-1), jnp.zeros((256,), jnp.float32)]).reshape(80, 128)
        flat = [opt_m, opt_v, master]
        state = [arr.reshape(OWN, 128) for arr in flat]
        frag = jnp.concatenate([arr[-HEAD * 128:] for arr in flat]).reshape(3 * HEAD, 128)
        g_nat, t_emb, t_attn, t_in, t_out, wvec, _ = exchange_call(grads, state, frag, vec)
        vec_flat = wvec.reshape(-1)
        wb_vecd = vec_flat[:9 * D].reshape(1, 9, D)
        wb_vecf = vec_flat[9 * D:9 * D + FF].reshape(1, FF)
        weights = (from_tiles(t_emb, VOCAB, D), from_tiles(t_attn, 4 * D, D), from_tiles(t_in, D, FF),
                   from_tiles(t_out, FF, D))
        y_out, m_new, v_new, w_new, wb_emb, wb_attn, wb_in, wb_out = ffn_call(
            tok_ids, act_in, t_emb.reshape(-1, 8, 128), weights[2], weights[3], wb_vecf, wb_vecd[0, 8:9],
            g_nat, state, weights)
        return (m_new.reshape(-1), v_new.reshape(-1), w_new.reshape(-1), wb_emb, wb_attn.reshape(1, 4, D, D),
                wb_in[None], wb_out[None], wb_vecd, wb_vecf, y_out)

    grad_specs = tuple(P(AXES, *([None] * (grad_rank - 1))) for grad_rank in GRAD_RANKS)
    in_specs = grad_specs + (P(AXES), P(AXES), P(AXES), P(AXES), P(AXES, None))
    out_specs = (P(AXES), P(AXES), P(AXES), P(), P(), P(), P(), P(), P(), P(AXES, None))
    return jax.shard_map(device_step, mesh=mesh, in_specs=in_specs, out_specs=out_specs, check_vma=False)
```

```python
import functools
import math
import jax
import jax.numpy as jnp
from jax import lax
from jax.experimental import pallas as pl
from jax.experimental.pallas import tpu as pltpu
from jax.sharding import PartitionSpec as P

LEARN_RATE = 0.002
BETA_ONE = 0.9
BETA_TWO = 0.95
ADAM_EPS = 1e-8
ADAM_STEP = 2
AXES = ("dz", "dy", "dx")
GRAD_RANKS = (3, 5, 4, 4, 4, 3)
MESH = pl.DeviceIdType.MESH

D = 768
FF = 3072
VOCAB = 2048
NCH = 22
TPC = 48
CROWS = 384
PART = NCH * CROWS
OWN = 8458
HEAD = 80
BOUNDS = (0, 32, 80, 128, 176)
OFFS = (0, 2, 4, 6, 8)
GROWS = 8784
SLOTS = 4 * NCH


def adam_math(grad, m_old, v_old, w_old):
    m_new = BETA_ONE * m_old + (1.0 - BETA_ONE) * grad
    v_new = BETA_TWO * v_old + (1.0 - BETA_TWO) * grad * grad
    m_hat = m_new / (1.0 - BETA_ONE ** ADAM_STEP)
    v_hat = v_new / (1.0 - BETA_TWO ** ADAM_STEP)
    w_new = w_old - LEARN_RATE * m_hat / (jnp.sqrt(v_hat) + ADAM_EPS)
    return m_new, v_new, w_new


def coords(index):
    return (index // 4, lax.rem(index // 2, 2), lax.rem(index, 2))


def engine_scratch(slots):
    f32, dma = jnp.float32, pltpu.SemaphoreType.DMA
    return [
        pltpu.VMEM((slots, TPC, 8, 128), f32),
        pltpu.VMEM((2, 4, TPC, 8, 128), f32),
        pltpu.VMEM((2 * NCH, TPC, 8, 128), f32),
        pltpu.VMEM((NCH, TPC, 8, 128), f32),
        pltpu.VMEM((2, CROWS, 128), f32),
        pltpu.VMEM((CROWS, 128), f32),
        pltpu.VMEM((2, 3, HEAD + CROWS, 128), f32),
        pltpu.VMEM((NCH, TPC, 8, 128), jnp.bfloat16),
        dma((slots,)), dma((slots,)), dma((2, 4)),
        dma((2 * NCH,)), dma((2 * NCH,)), dma((NCH,)), dma((NCH,)),
        dma((NCH,)), dma((slots,)), dma((slots,)), dma((slots,)), dma((slots,)),
        dma((NCH,)), dma((2, 3, 2)), dma((2,)), dma(()), dma(()),
    ]


class Engine:
    def __init__(self, grads, state, frag, g_nat, wbs, scratch):
        self.grads, self.state = grads, state
        self.frag, self.g_nat, self.wbs = frag, g_nat, wbs
        (self.rc, self.own, self.r1, self.r2, self.g_ch, self.w_ch, self.win, self.wbuf,
         self.d2d_s, self.d2d_r, self.own_sem, self.s1_s, self.s1_r, self.s2_s, self.s2_r,
         self.ay_s, self.ax_s, self.ac_s, self.ag_r, self.ac_r,
         self.wloc, self.win_sem, self.g_sem, self.tail_s, self.tail_r) = scratch
        dz, dy, dx = lax.axis_index("dz"), lax.axis_index("dy"), lax.axis_index("dx")
        self.me = dz * 4 + dy * 2 + dx
        self.p_core = (dz, dy, 1 - dx)
        core0 = dx == 0
        self.p_first = (jnp.where(core0, 1 - dz, dz), jnp.where(core0, dy, 1 - dy), dx)
        self.p_second = (jnp.where(core0, dz, 1 - dz), jnp.where(core0, 1 - dy, dy), dx)

        def part_of(is0, a, b):
            f, s = jnp.where(is0, dz, dy), jnp.where(is0, dy, dz)
            f = f if a == 0 else 1 - f
            s = s if b == 0 else 1 - s
            return jnp.where(is0, f * 4 + s * 2, s * 4 + f * 2) + jnp.where(is0 == core0, dx, 1 - dx)

        other0 = dx == 1
        self.mine = [part_of(core0, a, b) for a in (0, 1) for b in (0, 1)]
        self.theirs = [part_of(other0, a, b) for a in (0, 1) for b in (0, 1)]
        self.shift = self.me * 10

    def valid(self, j):
        return (j >= 0) & (j < NCH)

    def slot(self, part, j):
        return part // 2 * NCH + j

    def remote(self, src, dst, send, recv, to):
        return pltpu.make_async_remote_copy(src_ref=src, dst_ref=dst, send_sem=send, recv_sem=recv,
                                            device_id=to, device_id_type=MESH)

    def from_grad(self, part, j, go):
        at = part * NCH + j
        for lo, hi, ref in self.grads:
            @pl.when((at >= lo) & (at < hi))
            def _():
                go(ref.at[pl.ds((at - lo) * TPC, TPC)])

    def to_wb(self, part, j, go):
        at = part * NCH + j
        for lo, hi, ref in self.wbs:
            @pl.when((at >= lo) & (at < hi))
            def _():
                go(ref.at[at - lo])

    def own_load(self, j):
        buf = lax.rem(j, 2)
        for q in range(4):
            self.from_grad(self.mine[q], j, lambda src: pltpu.make_async_copy(
                src, self.own.at[buf, q], self.own_sem.at[buf, q]).start())

    def d2d_send(self, j):
        for part in self.theirs:
            s = self.slot(part, j)
            self.from_grad(part, j, lambda src: self.remote(
                src, self.rc.at[s], self.d2d_s.at[s], self.d2d_r.at[s], self.p_core).start())

    def landing(self, sem, ref):
        return self.remote(ref, ref, sem, sem, self.p_core)

    def step_one(self, s, b, j):
        n = b * NCH + j
        return self.remote(self.rc.at[s], self.r1.at[n], self.s1_s.at[n], self.s1_r.at[n], self.p_first)

    def step_two(self, j):
        return self.remote(self.r1.at[NCH + j], self.r2.at[j], self.s2_s.at[j], self.s2_r.at[j], self.p_second)

    def tail_copy(self):
        return self.remote(self.g_ch.at[0, pl.ds(0, HEAD)], self.g_nat.at[pl.ds(PART, HEAD)],
                           self.tail_s, self.tail_r, coords(jnp.maximum(self.me - 1, 0)))

    def window(self, j):
        c, buf = j, lax.rem(j, 2)
        rest = [pltpu.make_async_copy(
            src.at[pl.ds(pl.multiple_of(jnp.maximum(c * CROWS - HEAD, 0), 8), HEAD + CROWS)],
            self.win.at[buf, n], self.win_sem.at[buf, n, 0]) for n, src in enumerate(self.state)]
        zero = []
        for n, src in enumerate(self.state):
            zero.append(pltpu.make_async_copy(self.frag.at[pl.ds(HEAD * n, HEAD)], self.win.at[buf, n, pl.ds(0, HEAD)],
                                              self.win_sem.at[buf, n, 0]))
            zero.append(pltpu.make_async_copy(src.at[pl.ds(0, CROWS)], self.win.at[buf, n, pl.ds(HEAD, CROWS)],
                                              self.win_sem.at[buf, n, 1]))
        return c, rest, zero

    def window_do(self, j, what):
        c, rest, zero = self.window(j)

        @pl.when(c > 0)
        def _():
            for copy in rest:
                what(copy)

        @pl.when(c == 0)
        def _():
            for copy in zero:
                what(copy)

    def begin(self):
        self.own_load(jnp.int32(0))
        self.own_load(jnp.int32(1))

    def greet(self):
        barrier = pltpu.get_barrier_semaphore()
        for other in range(1, 8):
            pl.semaphore_signal(barrier, inc=1, device_id=coords(lax.rem(self.me + other, 8)), device_id_type=MESH)
        self.begin()
        pl.semaphore_wait(barrier, 7)
        for j in range(3):
            self.d2d_send(jnp.int32(j))

    def add_tiles(self, dst, src):
        def body(i, _):
            at = pl.ds(i * 8, 8)
            dst[at] = dst[at] + src[at]
            return 0
        lax.fori_loop(0, TPC // 8, body, 0)

    def stage_a(self, j):
        buf = lax.rem(j, 2)

        @pl.when(j + 3 < NCH)
        def _():
            self.d2d_send(j + 3)
        for q in (2, 3, 0, 1):
            s = self.slot(self.mine[q], j)
            pltpu.make_async_copy(self.own.at[buf, q], self.own.at[buf, q], self.own_sem.at[buf, q]).wait()
            self.landing(self.d2d_r.at[s], self.rc.at[s]).wait_recv()
            self.add_tiles(self.rc.at[s], self.own.at[buf, q])
            if q >= 2:
                self.step_one(s, q - 2, j).start()

        @pl.when(j + 2 < NCH)
        def _():
            self.own_load(j + 2)

    def stage_b(self, j):
        for b in (1, 0):
            s = self.slot(self.mine[b], j)
            self.step_one(s, b, j).wait_recv()
            self.add_tiles(self.r1.at[b * NCH + j], self.rc.at[s])
            if b == 1:
                self.step_two(j).start()

    def stage_c(self, j):
        me, s, i, c = self.me, self.slot(self.me, j), j, j
        buf = lax.rem(i, 2)
        at = me * NCH + c
        is_in = (at >= BOUNDS[2]) & (at < BOUNDS[3])
        g_store = pltpu.make_async_copy(self.g_ch.at[buf], self.g_nat.at[pl.ds(pl.multiple_of(c * CROWS, 8), CROWS)],
                                        self.g_sem.at[buf])
        self.step_two(j).wait_recv()

        @pl.when(i >= 2)
        def _():
            g_store.wait()

        @pl.when((i == 2) & (me > 0))
        def _():
            self.tail_copy().wait_send()

        def to_flat(width):
            def body(b, _):
                for n in range(width):
                    t = b * width + n
                    self.g_ch[buf, pl.ds(b * (8 * width) + n, 8, stride=width), :] = (
                        self.r2[i, t] + self.r1[i, t]) * 0.125
                return 0
            lax.fori_loop(0, TPC // width, body, 0)

        def to_tiles(width):
            def body(b, _):
                for n in range(width):
                    rows = self.w_ch[pl.ds(b * (8 * width) + n, 8, stride=width), :]
                    self.wbuf[i, b * width + n] = rows.astype(jnp.bfloat16)
                return 0
            lax.fori_loop(0, TPC // width, body, 0)

        @pl.when(is_in)
        def _():
            to_flat(24)

        @pl.when(jnp.logical_not(is_in))
        def _():
            to_flat(6)
        g_store.start()

        @pl.when((c == 0) & (me > 0))
        def _():
            self.tail_copy().start()
        self.window_do(j, lambda copy: copy.wait())

        def body(n, _):
            at = pl.ds(pl.multiple_of(n * 32, 8), 32)
            old = pl.ds(HEAD - self.shift + n * 32, 32)
            self.w_ch[at, :] = adam_math(self.g_ch[buf, at, :], self.win[buf, 0, old, :], self.win[buf, 1, old, :],
                                         self.win[buf, 2, old, :])[2]
            return 0
        lax.fori_loop(0, CROWS // 32, body, 0)

        @pl.when(is_in)
        def _():
            to_tiles(24)

        @pl.when(jnp.logical_not(is_in))
        def _():
            to_tiles(6)

        def send(dst):
            src = self.wbuf.at[i]
            self.remote(src, dst, self.ay_s.at[i], self.ag_r.at[s], self.p_second).start()
            self.remote(src, dst, self.ax_s.at[s], self.ag_r.at[s], self.p_first).start()
            self.remote(src, dst, self.ac_s.at[s], self.ac_r.at[s], self.p_core).start()
            pltpu.make_async_copy(src, dst, self.wloc.at[i]).start()
        self.to_wb(me, j, send)

    def stage_d(self, j):
        part = self.mine[1]
        s = self.slot(part, j)
        self.landing(self.ag_r.at[s], self.wbs[0][2].at[0]).wait_recv()

        def send(ref):
            self.remote(ref, ref, self.ax_s.at[s], self.ag_r.at[s], self.p_first).start()
            self.remote(ref, ref, self.ac_s.at[s], self.ac_r.at[s], self.p_core).start()
        self.to_wb(part, j, send)

    def stage_e(self, j):
        for part in (self.mine[2], self.mine[3]):
            s = self.slot(part, j)
            self.landing(self.ag_r.at[s], self.wbs[0][2].at[0]).wait_recv()
            self.to_wb(part, j, lambda ref: self.remote(
                ref, ref, self.ac_s.at[s], self.ac_r.at[s], self.p_core).start())

    def tick(self, t):
        for off, stage in zip(OFFS, (self.stage_a, self.stage_b, self.stage_c, self.stage_d, self.stage_e)):
            @pl.when(self.valid(t - off))
            def _():
                stage(t - off)
            if off == OFFS[2]:
                @pl.when(self.valid(t + 1 - off))
                def _():
                    self.window_do(t + 1 - off, lambda copy: copy.start())

    def drain(self):
        tile = self.wbs[0][2].at[0]

        def body(j, _):
            for part in self.theirs:
                s = self.slot(part, j)
                self.landing(self.d2d_s.at[s], self.rc.at[s]).wait_send()
                self.landing(self.ac_r.at[s], tile).wait_recv()
            for q, part in enumerate(self.mine):
                s = self.slot(part, j)
                self.landing(self.ac_s.at[s], tile).wait_send()
                if q >= 2:
                    self.step_one(s, q - 2, j).wait_send()
                else:
                    self.landing(self.ax_s.at[s], tile).wait_send()
            self.step_two(j).wait_send()
            self.landing(self.ay_s.at[j], tile).wait_send()
            pltpu.make_async_copy(tile, tile, self.wloc.at[j]).wait()
            return 0
        lax.fori_loop(0, NCH, body, 0)
        for buf in range(2):
            pltpu.make_async_copy(self.g_ch.at[buf], self.g_ch.at[buf], self.g_sem.at[buf]).wait()

        @pl.when(self.me < 7)
        def _():
            self.tail_copy().wait_recv()


def exchange_kernel(g_emb, g_attn, g_in, g_out, m_in, v_in, w_in, frag, vec,
                 g_nat, wb_emb, wb_attn, wb_in, wb_out, wvec_out, frag_got,
                 vecs, wvec, vwin, fr_s, fr_r, vc_s, vc_r, wv_s, wv_r, loc, vw_sem, *scratch):
    state = (m_in, v_in, w_in)
    span = lambda refs: [(BOUNDS[n], BOUNDS[n + 1], ref) for n, ref in enumerate(refs)]
    eng = Engine(span((g_emb, g_attn, g_in, g_out)), state, frag_got, g_nat,
                 span((wb_emb, wb_attn, wb_in, wb_out)), scratch)
    me = eng.me
    frag_copy = eng.remote(frag, frag_got, fr_s, fr_r, coords(jnp.minimum(me + 1, 7)))

    def vec_copy(n):
        return eng.remote(vec, vecs.at[n], vc_s, vc_r.at[n], coords(jnp.int32(7)))

    def wvec_copy(n):
        return eng.remote(wvec, wvec, wv_s.at[n], wv_r, coords(jnp.int32(n)))

    rows = OWN - 8368
    vwins = [pltpu.make_async_copy(src.at[pl.ds(8368, rows)], vwin.at[n, pl.ds(0, rows)], vw_sem.at[n])
             for n, src in enumerate(state)]
    eng.greet()

    @pl.when(me < 7)
    def _():
        frag_copy.start()
        vec_copy(me).start()

    @pl.when(me == 7)
    def _():
        for copy in vwins:
            copy.start()
        own_vec = pltpu.make_async_copy(vec, vecs.at[7], loc)
        own_vec.start()
        own_vec.wait()

    def step(t, _):
        @pl.when((t == OFFS[2] - 1) & (me > 0))
        def _():
            frag_copy.wait_recv()
        eng.tick(t)

        @pl.when((t == 8) & (me == 7))
        def _():
            for n in range(7):
                vec_copy(n).wait_recv()
            for copy in vwins:
                copy.wait()
            total = vecs[0]
            for n in range(1, 8):
                total = total + vecs[n]
            total = total * 0.125
            vecs[0] = total
            g_store = pltpu.make_async_copy(vecs.at[0], g_nat.at[pl.ds(PART, HEAD)], loc)
            g_store.start()
            old = pl.ds(10, HEAD)
            wvec[...] = adam_math(total, vwin[0, old, :], vwin[1, old, :], vwin[2, old, :])[2].astype(jnp.bfloat16)
            for n in range(7):
                wvec_copy(n).start()
            g_store.wait()
        return 0
    lax.fori_loop(0, NCH + OFFS[-1], step, 0)

    @pl.when(me < 7)
    def _():
        wvec_copy(0).wait_recv()
        frag_copy.wait_send()
        vec_copy(me).wait_send()

    @pl.when(me == 7)
    def _():
        for n in range(7):
            wvec_copy(n).wait_send()
    wv_store = pltpu.make_async_copy(wvec, wvec_out, loc)
    wv_store.start()
    eng.drain()
    wv_store.wait()


ANY = pl.BlockSpec(memory_space=pl.ANY)


def exchange_call(grads, state, frag, vec):
    f32, dma = jnp.float32, pltpu.SemaphoreType.DMA
    wb = lambda n: jax.ShapeDtypeStruct((BOUNDS[n + 1] - BOUNDS[n], TPC, 8, 128), jnp.bfloat16)
    return pl.pallas_call(
        exchange_kernel,
        out_shape=(jax.ShapeDtypeStruct((GROWS, 128), f32), wb(0), wb(1), wb(2), wb(3),
                   jax.ShapeDtypeStruct((HEAD, 128), jnp.bfloat16), jax.ShapeDtypeStruct((3 * HEAD, 128), f32)),
        in_specs=[ANY] * 9,
        out_specs=[ANY] * 7,
        scratch_shapes=[
            pltpu.VMEM((8, HEAD, 128), f32), pltpu.VMEM((HEAD, 128), jnp.bfloat16), pltpu.VMEM((3, 96, 128), f32),
            dma(()), dma(()), dma(()), dma((8,)), dma((7,)), dma(()), dma(()), dma((3,)),
        ] + engine_scratch(SLOTS),
        compiler_params=pltpu.CompilerParams(collective_id=0, has_side_effects=True, vmem_limit_bytes=62 << 20),
        name="adam_exchange",
    )(*grads, *state, frag, vec)


TM = 1024
FCH = 512
STATE_ROWS = 536
GELU_C = math.sqrt(2.0 / math.pi)


def gelu(x):
    half = 0.5 * x
    return half * jnp.tanh(x * (x * x * (GELU_C * 0.044715) + GELU_C)) + half


def ffn_kernel(ids, act, emb_t, win, wvec, m_ref, v_ref, w_ref, wout_hbm, g_hbm, attn_hbm,
               y_ref, m_out, v_out, w_out, vecd_out, vecf_out, emb_o, attn_o, in_o, out_o,
               table, rows, h_ref, u_ref, wout, g_ref, attn, vec_f, vecd, vecf, in_sem, out_sem):
    step = pl.program_id(0)
    last = pl.num_programs(0) - 1
    shift = (lax.axis_index("dz") * 4 + lax.axis_index("dy") * 2 + lax.axis_index("dx")) * 10
    loads = [pltpu.make_async_copy(src, dst, in_sem.at[n])
             for n, (src, dst) in enumerate(((wout_hbm, wout), (g_hbm, g_ref), (attn_hbm, attn)))]
    stores = [pltpu.make_async_copy(src, dst, out_sem.at[n])
              for n, (src, dst) in enumerate(((emb_t, emb_o), (win, in_o), (wout, out_o), (attn, attn_o)))]

    def pick_row(r, at):
        tok = ids[0, 0, r]
        rows[at, :] = table[pl.ds(pl.multiple_of(tok * 8, 8), 8), :]

    def build():
        for c in range(6):
            lanes = slice(c * 128, (c + 1) * 128)
            h_ref[:, lanes] = (rows[pl.ds(c, TM, stride=8), :] + act[:, lanes].astype(jnp.float32)).astype(jnp.bfloat16)

    @pl.when(step == 0)
    def _():
        for copy in loads + stores[:2]:
            copy.start()
        vec_f[...] = wvec[...].astype(jnp.float32)
        for n in range(54):
            vecd[n // 6:n // 6 + 1, n % 6 * 128:(n % 6 + 1) * 128] = vec_f[n:n + 1, :]
        for n in range(24):
            vecf[0:1, n * 128:(n + 1) * 128] = vec_f[54 + n:55 + n, :]
        vecd_out[...] = vecd[0:9, :].astype(jnp.bfloat16)
        vecf_out[...] = vecf[0:1, :].astype(jnp.bfloat16)

        def fill(b, _):
            for c in range(6):
                tile = emb_t[b * 6 + c].astype(jnp.float32) * math.sqrt(D)
                table[pl.ds(b * 64 + c, 8, stride=8), :] = tile
            return 0
        lax.fori_loop(0, VOCAB // 8, fill, 0)

        def pick(i, _):
            for k in range(16):
                r = i * 16 + k
                pick_row(r, pl.ds(pl.multiple_of(r * 8, 8), 8))
            return 0
        lax.fori_loop(0, TM // 16, pick, 0)
        build()

    @pl.when(step == 1)
    def _():
        for copy in loads:
            copy.wait()
        for copy in stores[2:]:
            copy.start()

    @pl.when(step > 0)
    def _():
        h = h_ref[...]
        count = FF // FCH
        for f in range(count):
            at = slice(f * FCH, (f + 1) * FCH)
            pre = jnp.dot(h, win[:, at], preferred_element_type=jnp.float32) + vecf[0:1, at]
            for r in range(f * TM // count, (f + 1) * TM // count):
                pick_row(r, slice(r * 8, r * 8 + 8))
            u_ref[:, at] = gelu(pre).astype(jnp.bfloat16)
        out = jnp.dot(u_ref[...], wout[...], preferred_element_type=jnp.float32)
        y_ref[...] = (out + vecd[8:9, :]).astype(jnp.bfloat16)
        build()
        grad = g_ref[pl.ds((step - 1) * STATE_ROWS + shift, STATE_ROWS), :]
        m_out[...], v_out[...], w_out[...] = adam_math(grad, m_ref[...], v_ref[...], w_ref[...])

    @pl.when(step == last)
    def _():
        for copy in stores:
            copy.wait()


def const(shape):
    return pl.BlockSpec(shape, lambda i: (0,) * len(shape), pipeline_mode=pl.Buffered(1))


def ffn_call(tok_ids, act_in, emb_t, win, wout, wvec, g_nat, attn_t, state):
    tiles = act_in.shape[0] // TM
    bf16, f32, dma = jnp.bfloat16, jnp.float32, pltpu.SemaphoreType.DMA
    before = lambda rows, cols: pl.BlockSpec((rows, cols), lambda i: (jnp.maximum(i - 1, 0), 0))
    after = lambda i: jnp.minimum(i, tiles - 1)
    kept = [before(STATE_ROWS, 128)] * 3
    like = lambda arr: jax.ShapeDtypeStruct(arr.shape, arr.dtype)
    return pl.pallas_call(
        ffn_kernel,
        grid=(tiles + 1,),
        out_shape=[like(act_in)] + [like(arr) for arr in state]
        + [jax.ShapeDtypeStruct((9, D), bf16), jax.ShapeDtypeStruct((1, FF), bf16)]
        + [like(arr) for arr in (emb_t, attn_t, win, wout)],
        in_specs=[
            pl.BlockSpec((1, 1, TM), lambda i: (after(i), 0, 0), memory_space=pltpu.SMEM),
            pl.BlockSpec((TM, D), lambda i: (after(i), 0)),
            const(emb_t.shape), const((D, FF)), const((HEAD, 128)),
        ] + kept + [ANY] * 3,
        out_specs=[before(TM, D)] + kept + [const((9, D)), const((1, FF))] + [ANY] * 4,
        scratch_shapes=[pltpu.VMEM((VOCAB * 8, 128), f32), pltpu.VMEM((TM * 8, 128), f32),
                        pltpu.VMEM((TM, D), bf16), pltpu.VMEM((TM, FF), bf16), pltpu.VMEM((FF, D), bf16),
                        pltpu.VMEM((GROWS, 128), f32), pltpu.VMEM(attn_t.shape, bf16),
                        pltpu.VMEM((HEAD, 128), f32), pltpu.VMEM((16, D), f32), pltpu.VMEM((8, FF), f32),
                        dma((3,)), dma((4,))],
        compiler_params=pltpu.CompilerParams(dimension_semantics=("arbitrary",), vmem_limit_bytes=63 << 20),
        name="ffn_and_state",
    )(tok_ids.reshape(tiles, 1, TM), act_in, emb_t, win, wvec, *state, wout, g_nat, attn_t)


def to_tiles(arr):
    rows, cols = arr.shape
    return arr.reshape(rows // 8, 8, cols // 128, 128).transpose(0, 2, 1, 3).reshape(rows * cols // 1024, 8, 128)


def from_tiles(tiles, rows, cols):
    return tiles.reshape(rows // 8, cols // 128, 8, 128).transpose(0, 2, 1, 3).reshape(rows, cols)


def solution(mesh):
    def device_step(g_emb, g_attn, g_in, g_out, g_vecd, g_vecf, opt_m, opt_v, master, tok_ids, act_in):
        grads = [to_tiles(g_emb[0]), to_tiles(g_attn.reshape(4 * D, D)), to_tiles(g_in[0, 0]), to_tiles(g_out[0, 0])]
        vec = jnp.concatenate([g_vecd.reshape(-1), g_vecf.reshape(-1), jnp.zeros((256,), jnp.float32)]).reshape(80, 128)
        flat = [opt_m, opt_v, master]
        state = [arr.reshape(OWN, 128) for arr in flat]
        frag = jnp.concatenate([arr[-HEAD * 128:] for arr in flat]).reshape(3 * HEAD, 128)
        g_nat, t_emb, t_attn, t_in, t_out, wvec, _ = exchange_call(grads, state, frag, vec)
        y_out, m_new, v_new, w_new, wb_vecd, wb_vecf, t_emb, t_attn, wb_in, wb_out = ffn_call(
            tok_ids, act_in, t_emb.reshape(-1, 8, 128), from_tiles(t_in, D, FF), from_tiles(t_out, FF, D), wvec,
            g_nat, t_attn.reshape(-1, 8, 128), state)
        return (m_new.reshape(-1), v_new.reshape(-1), w_new.reshape(-1), from_tiles(t_emb, VOCAB, D),
                from_tiles(t_attn, 4 * D, D).reshape(1, 4, D, D), wb_in[None], wb_out[None], wb_vecd[None], wb_vecf,
                y_out)

    grad_specs = tuple(P(AXES, *([None] * (grad_rank - 1))) for grad_rank in GRAD_RANKS)
    in_specs = grad_specs + (P(AXES), P(AXES), P(AXES), P(AXES), P(AXES, None))
    out_specs = (P(AXES), P(AXES), P(AXES), P(), P(), P(), P(), P(), P(), P(AXES, None))
    return jax.shard_map(device_step, mesh=mesh, in_specs=in_specs, out_specs=out_specs, check_vma=False)
```

```python
import functools
import math
import jax
import jax.numpy as jnp
from jax import lax
from jax.experimental import pallas as pl
from jax.experimental.pallas import tpu as pltpu
from jax.sharding import PartitionSpec as P

LEARN_RATE = 0.002
BETA_ONE = 0.9
BETA_TWO = 0.95
ADAM_EPS = 1e-8
ADAM_STEP = 2
AXES = ("dz", "dy", "dx")
GRAD_RANKS = (3, 5, 4, 4, 4, 3)
MESH = pl.DeviceIdType.MESH

D = 768
FF = 3072
VOCAB = 2048
NCH = 22
TPC = 48
CROWS = 384
PART = NCH * CROWS
OWN = 8458
HEAD = 80
BOUNDS = (0, 32, 80, 128, 176)
OFFS = (0, 2, 4, 6, 8)
GROWS = 8784
SLOTS = 4 * NCH


def adam_math(grad, m_old, v_old, w_old):
    m_new = BETA_ONE * m_old + (1.0 - BETA_ONE) * grad
    v_new = BETA_TWO * v_old + (1.0 - BETA_TWO) * grad * grad
    m_hat = m_new / (1.0 - BETA_ONE ** ADAM_STEP)
    v_hat = v_new / (1.0 - BETA_TWO ** ADAM_STEP)
    w_new = w_old - LEARN_RATE * m_hat / (jnp.sqrt(v_hat) + ADAM_EPS)
    return m_new, v_new, w_new


def coords(index):
    return (index // 4, lax.rem(index // 2, 2), lax.rem(index, 2))


def engine_scratch(slots):
    f32, dma = jnp.float32, pltpu.SemaphoreType.DMA
    return [
        pltpu.VMEM((slots, TPC, 8, 128), f32),
        pltpu.VMEM((2, 4, TPC, 8, 128), f32),
        pltpu.VMEM((2 * NCH, TPC, 8, 128), f32),
        pltpu.VMEM((NCH, TPC, 8, 128), f32),
        pltpu.VMEM((2, CROWS, 128), f32),
        pltpu.VMEM((CROWS, 128), f32),
        pltpu.VMEM((2, 3, HEAD + CROWS, 128), f32),
        pltpu.VMEM((NCH, TPC, 8, 128), jnp.bfloat16),
        dma((slots,)), dma((slots,)), dma((2, 4)),
        dma((2 * NCH,)), dma((2 * NCH,)), dma((NCH,)), dma((NCH,)),
        dma((NCH,)), dma((slots,)), dma((slots,)), dma((slots,)), dma((slots,)),
        dma((NCH,)), dma((2, 3, 2)), dma((2,)), dma(()), dma(()),
    ]


class Engine:
    def __init__(self, grads, state, frag, g_nat, wbs, scratch):
        self.grads, self.state = grads, state
        self.frag, self.g_nat, self.wbs = frag, g_nat, wbs
        (self.rc, self.own, self.r1, self.r2, self.g_ch, self.w_ch, self.win, self.wbuf,
         self.d2d_s, self.d2d_r, self.own_sem, self.s1_s, self.s1_r, self.s2_s, self.s2_r,
         self.ay_s, self.ax_s, self.ac_s, self.ag_r, self.ac_r,
         self.wloc, self.win_sem, self.g_sem, self.tail_s, self.tail_r) = scratch
        dz, dy, dx = lax.axis_index("dz"), lax.axis_index("dy"), lax.axis_index("dx")
        self.me = dz * 4 + dy * 2 + dx
        self.p_core = (dz, dy, 1 - dx)
        core0 = dx == 0
        self.p_first = (jnp.where(core0, 1 - dz, dz), jnp.where(core0, dy, 1 - dy), dx)
        self.p_second = (jnp.where(core0, dz, 1 - dz), jnp.where(core0, 1 - dy, dy), dx)

        def part_of(is0, a, b):
            f, s = jnp.where(is0, dz, dy), jnp.where(is0, dy, dz)
            f = f if a == 0 else 1 - f
            s = s if b == 0 else 1 - s
            return jnp.where(is0, f * 4 + s * 2, s * 4 + f * 2) + jnp.where(is0 == core0, dx, 1 - dx)

        other0 = dx == 1
        self.mine = [part_of(core0, a, b) for a in (0, 1) for b in (0, 1)]
        self.theirs = [part_of(other0, a, b) for a in (0, 1) for b in (0, 1)]
        self.shift = self.me * 10

    def valid(self, j):
        return (j >= 0) & (j < NCH)

    def slot(self, part, j):
        return part // 2 * NCH + j

    def remote(self, src, dst, send, recv, to):
        return pltpu.make_async_remote_copy(src_ref=src, dst_ref=dst, send_sem=send, recv_sem=recv,
                                            device_id=to, device_id_type=MESH)

    def from_grad(self, part, j, go):
        at = part * NCH + j
        for lo, hi, ref in self.grads:
            @pl.when((at >= lo) & (at < hi))
            def _():
                go(ref.at[pl.ds((at - lo) * TPC, TPC)])

    def to_wb(self, part, j, go):
        at = part * NCH + j
        for lo, hi, ref in self.wbs:
            @pl.when((at >= lo) & (at < hi))
            def _():
                go(ref.at[at - lo])

    def own_load(self, j):
        buf = lax.rem(j, 2)
        for q in range(4):
            self.from_grad(self.mine[q], j, lambda src: pltpu.make_async_copy(
                src, self.own.at[buf, q], self.own_sem.at[buf, q]).start())

    def d2d_send(self, j):
        for part in self.theirs:
            s = self.slot(part, j)
            self.from_grad(part, j, lambda src: self.remote(
                src, self.rc.at[s], self.d2d_s.at[s], self.d2d_r.at[s], self.p_core).start())

    def landing(self, sem, ref):
        return self.remote(ref, ref, sem, sem, self.p_core)

    def step_one(self, s, b, j):
        n = b * NCH + j
        return self.remote(self.rc.at[s], self.r1.at[n], self.s1_s.at[n], self.s1_r.at[n], self.p_first)

    def step_two(self, j):
        return self.remote(self.r1.at[NCH + j], self.r2.at[j], self.s2_s.at[j], self.s2_r.at[j], self.p_second)

    def tail_copy(self):
        return self.remote(self.g_ch.at[0, pl.ds(0, HEAD)], self.g_nat.at[pl.ds(PART, HEAD)],
                           self.tail_s, self.tail_r, coords(jnp.maximum(self.me - 1, 0)))

    def window(self, j):
        c, buf = j, lax.rem(j, 2)
        rest = [pltpu.make_async_copy(
            src.at[pl.ds(pl.multiple_of(jnp.maximum(c * CROWS - HEAD, 0), 8), HEAD + CROWS)],
            self.win.at[buf, n], self.win_sem.at[buf, n, 0]) for n, src in enumerate(self.state)]
        zero = []
        for n, src in enumerate(self.state):
            zero.append(pltpu.make_async_copy(self.frag.at[pl.ds(HEAD * n, HEAD)], self.win.at[buf, n, pl.ds(0, HEAD)],
                                              self.win_sem.at[buf, n, 0]))
            zero.append(pltpu.make_async_copy(src.at[pl.ds(0, CROWS)], self.win.at[buf, n, pl.ds(HEAD, CROWS)],
                                              self.win_sem.at[buf, n, 1]))
        return c, rest, zero

    def window_do(self, j, what):
        c, rest, zero = self.window(j)

        @pl.when(c > 0)
        def _():
            for copy in rest:
                what(copy)

        @pl.when(c == 0)
        def _():
            for copy in zero:
                what(copy)

    def begin(self):
        self.own_load(jnp.int32(0))
        self.own_load(jnp.int32(1))

    def greet(self):
        barrier = pltpu.get_barrier_semaphore()
        for other in range(1, 8):
            pl.semaphore_signal(barrier, inc=1, device_id=coords(lax.rem(self.me + other, 8)), device_id_type=MESH)
        self.begin()
        pl.semaphore_wait(barrier, 7)
        for j in range(3):
            self.d2d_send(jnp.int32(j))

    def add_tiles(self, dst, src):
        def body(i, _):
            at = pl.ds(i * 8, 8)
            dst[at] = dst[at] + src[at]
            return 0
        lax.fori_loop(0, TPC // 8, body, 0)

    def stage_a(self, j):
        buf = lax.rem(j, 2)

        @pl.when(j + 3 < NCH)
        def _():
            self.d2d_send(j + 3)
        for q in (2, 3, 0, 1):
            s = self.slot(self.mine[q], j)
            pltpu.make_async_copy(self.own.at[buf, q], self.own.at[buf, q], self.own_sem.at[buf, q]).wait()
            self.landing(self.d2d_r.at[s], self.rc.at[s]).wait_recv()
            self.add_tiles(self.rc.at[s], self.own.at[buf, q])
            if q >= 2:
                self.step_one(s, q - 2, j).start()

        @pl.when(j + 2 < NCH)
        def _():
            self.own_load(j + 2)

    def stage_b(self, j):
        for b in (1, 0):
            s = self.slot(self.mine[b], j)
            self.step_one(s, b, j).wait_recv()
            self.add_tiles(self.r1.at[b * NCH + j], self.rc.at[s])
            if b == 1:
                self.step_two(j).start()

    def stage_c(self, j):
        me, s, i, c = self.me, self.slot(self.me, j), j, j
        buf = lax.rem(i, 2)
        at = me * NCH + c
        is_in = (at >= BOUNDS[2]) & (at < BOUNDS[3])
        g_store = pltpu.make_async_copy(self.g_ch.at[buf], self.g_nat.at[pl.ds(pl.multiple_of(c * CROWS, 8), CROWS)],
                                        self.g_sem.at[buf])
        self.step_two(j).wait_recv()

        @pl.when(i >= 2)
        def _():
            g_store.wait()

        @pl.when((i == 2) & (me > 0))
        def _():
            self.tail_copy().wait_send()

        def to_flat(width):
            def body(b, _):
                for n in range(width):
                    t = b * width + n
                    self.g_ch[buf, pl.ds(b * (8 * width) + n, 8, stride=width), :] = (
                        self.r2[i, t] + self.r1[i, t]) * 0.125
                return 0
            lax.fori_loop(0, TPC // width, body, 0)

        def to_tiles(width):
            def body(b, _):
                for n in range(width):
                    rows = self.w_ch[pl.ds(b * (8 * width) + n, 8, stride=width), :]
                    self.wbuf[i, b * width + n] = rows.astype(jnp.bfloat16)
                return 0
            lax.fori_loop(0, TPC // width, body, 0)

        @pl.when(is_in)
        def _():
            to_flat(24)

        @pl.when(jnp.logical_not(is_in))
        def _():
            to_flat(6)
        g_store.start()

        @pl.when((c == 0) & (me > 0))
        def _():
            self.tail_copy().start()
        self.window_do(j, lambda copy: copy.wait())

        def body(n, _):
            at = pl.ds(pl.multiple_of(n * 32, 8), 32)
            old = pl.ds(HEAD - self.shift + n * 32, 32)
            self.w_ch[at, :] = adam_math(self.g_ch[buf, at, :], self.win[buf, 0, old, :], self.win[buf, 1, old, :],
                                         self.win[buf, 2, old, :])[2]
            return 0
        lax.fori_loop(0, CROWS // 32, body, 0)

        @pl.when(is_in)
        def _():
            to_tiles(24)

        @pl.when(jnp.logical_not(is_in))
        def _():
            to_tiles(6)

        def send(dst):
            src = self.wbuf.at[i]
            self.remote(src, dst, self.ay_s.at[i], self.ag_r.at[s], self.p_second).start()
            self.remote(src, dst, self.ax_s.at[s], self.ag_r.at[s], self.p_first).start()
            self.remote(src, dst, self.ac_s.at[s], self.ac_r.at[s], self.p_core).start()
            pltpu.make_async_copy(src, dst, self.wloc.at[i]).start()
        self.to_wb(me, j, send)

    def stage_d(self, j):
        part = self.mine[1]
        s = self.slot(part, j)
        self.landing(self.ag_r.at[s], self.wbs[0][2].at[0]).wait_recv()

        def send(ref):
            self.remote(ref, ref, self.ax_s.at[s], self.ag_r.at[s], self.p_first).start()
            self.remote(ref, ref, self.ac_s.at[s], self.ac_r.at[s], self.p_core).start()
        self.to_wb(part, j, send)

    def stage_e(self, j):
        for part in (self.mine[2], self.mine[3]):
            s = self.slot(part, j)
            self.landing(self.ag_r.at[s], self.wbs[0][2].at[0]).wait_recv()
            self.to_wb(part, j, lambda ref: self.remote(
                ref, ref, self.ac_s.at[s], self.ac_r.at[s], self.p_core).start())

    def tick(self, t):
        for off, stage in zip(OFFS, (self.stage_a, self.stage_b, self.stage_c, self.stage_d, self.stage_e)):
            @pl.when(self.valid(t - off))
            def _():
                stage(t - off)
            if off == OFFS[2]:
                @pl.when(self.valid(t + 1 - off))
                def _():
                    self.window_do(t + 1 - off, lambda copy: copy.start())

    def drain(self):
        tile = self.wbs[0][2].at[0]

        def body(j, _):
            for part in self.theirs:
                s = self.slot(part, j)
                self.landing(self.d2d_s.at[s], self.rc.at[s]).wait_send()
                self.landing(self.ac_r.at[s], tile).wait_recv()
            for q, part in enumerate(self.mine):
                s = self.slot(part, j)
                self.landing(self.ac_s.at[s], tile).wait_send()
                if q >= 2:
                    self.step_one(s, q - 2, j).wait_send()
                else:
                    self.landing(self.ax_s.at[s], tile).wait_send()
            self.step_two(j).wait_send()
            self.landing(self.ay_s.at[j], tile).wait_send()
            pltpu.make_async_copy(tile, tile, self.wloc.at[j]).wait()
            return 0
        lax.fori_loop(0, NCH, body, 0)
        for buf in range(2):
            pltpu.make_async_copy(self.g_ch.at[buf], self.g_ch.at[buf], self.g_sem.at[buf]).wait()

        @pl.when(self.me < 7)
        def _():
            self.tail_copy().wait_recv()


def exchange_kernel(g_emb, g_attn, g_in, g_out, m_in, v_in, w_in, vec,
                 g_nat, wb_emb, wb_attn, wb_in, wb_out, wvec_out, frag_got,
                 vecs, wvec, vwin, frag, fr_s, fr_r, vc_s, vc_r, wv_s, wv_r, loc, vw_sem, *scratch):
    state = (m_in, v_in, w_in)
    span = lambda refs: [(BOUNDS[n], BOUNDS[n + 1], ref) for n, ref in enumerate(refs)]
    eng = Engine(span((g_emb, g_attn, g_in, g_out)), state, frag_got, g_nat,
                 span((wb_emb, wb_attn, wb_in, wb_out)), scratch)
    me = eng.me
    frag_copy = eng.remote(frag, frag_got, fr_s, fr_r, coords(jnp.minimum(me + 1, 7)))

    def vec_copy(n):
        return eng.remote(vec, vecs.at[n], vc_s, vc_r.at[n], coords(jnp.int32(7)))

    def wvec_copy(n):
        return eng.remote(wvec, wvec, wv_s.at[n], wv_r, coords(jnp.int32(n)))

    rows = OWN - 8368
    vwins = [pltpu.make_async_copy(src.at[pl.ds(8368, rows)], vwin.at[n, pl.ds(0, rows)], vw_sem.at[n])
             for n, src in enumerate(state)]
    for copy in vwins:
        copy.start()
    eng.greet()
    for n, copy in enumerate(vwins):
        copy.wait()
        frag[pl.ds(n * HEAD, HEAD), :] = vwin[n, pl.ds(10, HEAD), :]

    @pl.when(me < 7)
    def _():
        frag_copy.start()
        vec_copy(me).start()

    @pl.when(me == 7)
    def _():
        own_vec = pltpu.make_async_copy(vec, vecs.at[7], loc)
        own_vec.start()
        own_vec.wait()

    def step(t, _):
        @pl.when((t == OFFS[2] - 1) & (me > 0))
        def _():
            frag_copy.wait_recv()
        eng.tick(t)

        @pl.when((t == 8) & (me == 7))
        def _():
            for n in range(7):
                vec_copy(n).wait_recv()
            total = vecs[0]
            for n in range(1, 8):
                total = total + vecs[n]
            total = total * 0.125
            vecs[0] = total
            g_store = pltpu.make_async_copy(vecs.at[0], g_nat.at[pl.ds(PART, HEAD)], loc)
            g_store.start()
            old = pl.ds(10, HEAD)
            wvec[...] = adam_math(total, vwin[0, old, :], vwin[1, old, :], vwin[2, old, :])[2].astype(jnp.bfloat16)
            for n in range(7):
                wvec_copy(n).start()
            g_store.wait()
        return 0
    lax.fori_loop(0, NCH + OFFS[-1], step, 0)

    @pl.when(me < 7)
    def _():
        wvec_copy(0).wait_recv()
        frag_copy.wait_send()
        vec_copy(me).wait_send()

    @pl.when(me == 7)
    def _():
        for n in range(7):
            wvec_copy(n).wait_send()
    wv_store = pltpu.make_async_copy(wvec, wvec_out, loc)
    wv_store.start()
    eng.drain()
    wv_store.wait()


ANY = pl.BlockSpec(memory_space=pl.ANY)


def exchange_call(grads, state, vec):
    f32, dma = jnp.float32, pltpu.SemaphoreType.DMA
    wb = lambda n: jax.ShapeDtypeStruct((BOUNDS[n + 1] - BOUNDS[n], TPC, 8, 128), jnp.bfloat16)
    return pl.pallas_call(
        exchange_kernel,
        out_shape=(jax.ShapeDtypeStruct((GROWS, 128), f32), wb(0), wb(1), wb(2), wb(3),
                   jax.ShapeDtypeStruct((HEAD, 128), jnp.bfloat16), jax.ShapeDtypeStruct((3 * HEAD, 128), f32)),
        in_specs=[ANY] * 8,
        out_specs=[ANY] * 7,
        scratch_shapes=[
            pltpu.VMEM((8, HEAD, 128), f32), pltpu.VMEM((HEAD, 128), jnp.bfloat16), pltpu.VMEM((3, 96, 128), f32), pltpu.VMEM((3 * HEAD, 128), f32),
            dma(()), dma(()), dma(()), dma((8,)), dma((7,)), dma(()), dma(()), dma((3,)),
        ] + engine_scratch(SLOTS),
        compiler_params=pltpu.CompilerParams(collective_id=0, has_side_effects=True, vmem_limit_bytes=62 << 20),
        name="adam_exchange",
    )(*grads, *state, vec)


TM = 1024
FCH = 1024
STATE_ROWS = 536
GELU_C = math.sqrt(2.0 / math.pi)


def gelu(x):
    half = 0.5 * x
    return half * jnp.tanh(x * (x * x * (GELU_C * 0.044715) + GELU_C)) + half


def ffn_kernel(ids, act, emb_t, win, wvec, m_ref, v_ref, w_ref, wout_hbm, g_hbm, attn_hbm,
               y_ref, m_out, v_out, w_out, vecd_out, vecf_out, emb_o, attn_o, in_o, out_o,
               table, rows, h_ref, u_ref, wout, g_ref, attn, vec_f, vecd, vecf, in_sem, out_sem):
    step = pl.program_id(0)
    last = pl.num_programs(0) - 1
    shift = (lax.axis_index("dz") * 4 + lax.axis_index("dy") * 2 + lax.axis_index("dx")) * 10
    loads = [pltpu.make_async_copy(src, dst, in_sem.at[n])
             for n, (src, dst) in enumerate(((wout_hbm, wout), (g_hbm, g_ref), (attn_hbm, attn)))]
    stores = [pltpu.make_async_copy(src, dst, out_sem.at[n])
              for n, (src, dst) in enumerate(((emb_t, emb_o), (win, in_o), (wout, out_o), (attn, attn_o)))]

    def pick_row(r, at):
        tok = ids[0, 0, r]
        rows[at, :] = table[pl.ds(pl.multiple_of(tok * 8, 8), 8), :]

    def build():
        for c in range(6):
            lanes = slice(c * 128, (c + 1) * 128)
            h_ref[:, lanes] = (rows[pl.ds(c, TM, stride=8), :] + act[:, lanes].astype(jnp.float32)).astype(jnp.bfloat16)

    @pl.when(step == 0)
    def _():
        for copy in loads + stores[:2]:
            copy.start()
        vec_f[...] = wvec[...].astype(jnp.float32)
        for n in range(54):
            vecd[n // 6:n // 6 + 1, n % 6 * 128:(n % 6 + 1) * 128] = vec_f[n:n + 1, :]
        for n in range(24):
            vecf[0:1, n * 128:(n + 1) * 128] = vec_f[54 + n:55 + n, :]
        vecd_out[...] = vecd[0:9, :].astype(jnp.bfloat16)
        vecf_out[...] = vecf[0:1, :].astype(jnp.bfloat16)

        def fill(b, _):
            for c in range(6):
                tile = emb_t[b * 6 + c].astype(jnp.float32) * math.sqrt(D)
                table[pl.ds(b * 64 + c, 8, stride=8), :] = tile
            return 0
        lax.fori_loop(0, VOCAB // 8, fill, 0)

        def pick(i, _):
            for k in range(16):
                r = i * 16 + k
                pick_row(r, pl.ds(pl.multiple_of(r * 8, 8), 8))
            return 0
        lax.fori_loop(0, TM // 16, pick, 0)
        build()

    @pl.when(step == 1)
    def _():
        for copy in loads:
            copy.wait()
        for copy in stores[2:]:
            copy.start()

    @pl.when(step > 0)
    def _():
        h = h_ref[...]
        count = FF // FCH
        for f in range(count):
            at = slice(f * FCH, (f + 1) * FCH)
            pre = jnp.dot(h, win[:, at], preferred_element_type=jnp.float32) + vecf[0:1, at]
            for r in range(f * TM // count, (f + 1) * TM // count):
                pick_row(r, slice(r * 8, r * 8 + 8))
            u_ref[:, at] = gelu(pre).astype(jnp.bfloat16)
        out = jnp.dot(u_ref[...], wout[...], preferred_element_type=jnp.float32)
        y_ref[...] = (out + vecd[8:9, :]).astype(jnp.bfloat16)
        build()
        grad = g_ref[pl.ds((step - 1) * STATE_ROWS + shift, STATE_ROWS), :]
        m_out[...], v_out[...], w_out[...] = adam_math(grad, m_ref[...], v_ref[...], w_ref[...])

    @pl.when(step == last)
    def _():
        for copy in stores:
            copy.wait()


def const(shape):
    return pl.BlockSpec(shape, lambda i: (0,) * len(shape), pipeline_mode=pl.Buffered(1))


def ffn_call(tok_ids, act_in, emb_t, win, wout, wvec, g_nat, attn_t, state):
    tiles = act_in.shape[0] // TM
    bf16, f32, dma = jnp.bfloat16, jnp.float32, pltpu.SemaphoreType.DMA
    before = lambda rows, cols: pl.BlockSpec((rows, cols), lambda i: (jnp.maximum(i - 1, 0), 0))
    after = lambda i: jnp.minimum(i, tiles - 1)
    kept = [before(STATE_ROWS, 128)] * 3
    like = lambda arr: jax.ShapeDtypeStruct(arr.shape, arr.dtype)
    return pl.pallas_call(
        ffn_kernel,
        grid=(tiles + 1,),
        out_shape=[like(act_in)] + [like(arr) for arr in state]
        + [jax.ShapeDtypeStruct((9, D), bf16), jax.ShapeDtypeStruct((1, FF), bf16)]
        + [like(arr) for arr in (emb_t, attn_t, win, wout)],
        in_specs=[
            pl.BlockSpec((1, 1, TM), lambda i: (after(i), 0, 0), memory_space=pltpu.SMEM),
            pl.BlockSpec((TM, D), lambda i: (after(i), 0)),
            const(emb_t.shape), const((D, FF)), const((HEAD, 128)),
        ] + kept + [ANY] * 3,
        out_specs=[before(TM, D)] + kept + [const((9, D)), const((1, FF))] + [ANY] * 4,
        scratch_shapes=[pltpu.VMEM((VOCAB * 8, 128), f32), pltpu.VMEM((TM * 8, 128), f32),
                        pltpu.VMEM((TM, D), bf16), pltpu.VMEM((TM, FF), bf16), pltpu.VMEM((FF, D), bf16),
                        pltpu.VMEM((GROWS, 128), f32), pltpu.VMEM(attn_t.shape, bf16),
                        pltpu.VMEM((HEAD, 128), f32), pltpu.VMEM((16, D), f32), pltpu.VMEM((8, FF), f32),
                        dma((3,)), dma((4,))],
        compiler_params=pltpu.CompilerParams(dimension_semantics=("arbitrary",), vmem_limit_bytes=63 << 20),
        name="ffn_and_state",
    )(tok_ids.reshape(tiles, 1, TM), act_in, emb_t, win, wvec, *state, wout, g_nat, attn_t)


def to_tiles(arr):
    rows, cols = arr.shape
    return arr.reshape(rows // 8, 8, cols // 128, 128).transpose(0, 2, 1, 3).reshape(rows * cols // 1024, 8, 128)


def from_tiles(tiles, rows, cols):
    return tiles.reshape(rows // 8, cols // 128, 8, 128).transpose(0, 2, 1, 3).reshape(rows, cols)


def solution(mesh):
    def device_step(g_emb, g_attn, g_in, g_out, g_vecd, g_vecf, opt_m, opt_v, master, tok_ids, act_in):
        grads = [to_tiles(g_emb[0]), to_tiles(g_attn.reshape(4 * D, D)), to_tiles(g_in[0, 0]), to_tiles(g_out[0, 0])]
        vec = jnp.concatenate([g_vecd.reshape(-1), g_vecf.reshape(-1), jnp.zeros((256,), jnp.float32)]).reshape(80, 128)
        flat = [opt_m, opt_v, master]
        state = [arr.reshape(OWN, 128) for arr in flat]
        g_nat, t_emb, t_attn, t_in, t_out, wvec, _ = exchange_call(grads, state, vec)
        y_out, m_new, v_new, w_new, wb_vecd, wb_vecf, t_emb, t_attn, wb_in, wb_out = ffn_call(
            tok_ids, act_in, t_emb.reshape(-1, 8, 128), from_tiles(t_in, D, FF), from_tiles(t_out, FF, D), wvec,
            g_nat, t_attn.reshape(-1, 8, 128), state)
        return (m_new.reshape(-1), v_new.reshape(-1), w_new.reshape(-1), from_tiles(t_emb, VOCAB, D),
                from_tiles(t_attn, 4 * D, D).reshape(1, 4, D, D), wb_in[None], wb_out[None], wb_vecd[None], wb_vecf,
                y_out)

    grad_specs = tuple(P(AXES, *([None] * (grad_rank - 1))) for grad_rank in GRAD_RANKS)
    in_specs = grad_specs + (P(AXES), P(AXES), P(AXES), P(AXES), P(AXES, None))
    out_specs = (P(AXES), P(AXES), P(AXES), P(), P(), P(), P(), P(), P(), P(AXES, None))
    return jax.shard_map(device_step, mesh=mesh, in_specs=in_specs, out_specs=out_specs, check_vma=False)
```
